16 devices in a mesh: dp: 2 (over y, z), stage: 8 (over x, core).
Axes of the slice: x: 4, y: 2, z: 1, core: 2. Of those that a mesh axis runs over, the one named last changes fastest.
The devices are a block of a 4x4x8 slice.
Arguments:
- token_ids: int32 [16, 256], P('dp'), parts along dimension 0
- label_ids: int32 [16, 256], P('dp'), parts along dimension 0
- label2_ids: int32 [16, 256], P('dp'), parts along dimension 0
- embed_table: bfloat16 [32128, 512], replicated
- w_up: bfloat16 [8, 512, 4096], P('stage')
- w_down: bfloat16 [8, 4096, 512], P('stage')
- mtp_up: bfloat16 [512, 4096], replicated
- mtp_down: bfloat16 [4096, 512], replicated
Outputs:
- output 1: float32 [2], P('dp'), parts along dimension 0
- output 2: float32 [16, 512, 4096], P(('dp', 'stage')), parts along dimension 0
- output 3: float32 [16, 4096, 512], P(('dp', 'stage')), parts along dimension 0
- output 4: float32 [64256, 512], P('dp'), parts along dimension 0
There are 2 independent parts. The reference program is written for one: setup_inputs(seed, part) draws one part's arguments, and reference() takes and returns one part's arrays. A program takes and returns all parts, laid end to end along the dimension named above; an argument that names none is the same for every part.
All inputs are finite; a program needn't handle non-finite values.
Results may differ from the reference program's by a relative error of at most 0.0140777.
Values are sent between devices in bfloat16 or wider.
A program may use at most 768 MiB of HBM per device.

```python
import jax
import jax.numpy as jnp
from jax import lax

VOCAB_SIZE = 32128
MODEL_WIDTH = 512
HIDDEN_WIDTH = 4096
MICRO_BATCHES = 8
SEQ_TOKENS = 256
NUM_STAGES = 8
HOT_RANGE = min(VOCAB_SIZE, 512)
EPS_NORM = 1e-6


def draw_ids(key):
    key_wide, key_hot, key_pick = jax.random.split(key, 3)
    id_shape = (MICRO_BATCHES, SEQ_TOKENS + 2)
    wide_ids = jax.random.randint(key_wide, id_shape, 0, VOCAB_SIZE)
    hot_ids = jax.random.randint(key_hot, id_shape, 0, HOT_RANGE)
    pick_hot = jax.random.randint(key_pick, id_shape, 0, 2)
    id_stream = jnp.where(pick_hot == 0, wide_ids, hot_ids)
    id_stream = id_stream.at[0, 0].set(VOCAB_SIZE - 1).at[0, 1].set(0)
    return id_stream[:, :SEQ_TOKENS], id_stream[:, 1:SEQ_TOKENS + 1], id_stream[:, 2:]


def setup_inputs(seed: int = 0, part: int = 0) -> dict:
    base_key = jax.random.key(seed)
    part_key = jax.random.fold_in(base_key, part)
    token_ids, label_ids, label2_ids = draw_ids(jax.random.fold_in(part_key, 1))
    key_emb, key_up, key_down, key_mup, key_mdown = jax.random.split(jax.random.fold_in(base_key, 2), 5)
    embed_table = jax.random.normal(key_emb, (VOCAB_SIZE, MODEL_WIDTH), jnp.float32).astype(jnp.bfloat16)
    w_up = (jax.random.normal(key_up, (NUM_STAGES, MODEL_WIDTH, HIDDEN_WIDTH), jnp.float32) * MODEL_WIDTH ** -0.5).astype(jnp.bfloat16)
    w_down = (jax.random.normal(key_down, (NUM_STAGES, HIDDEN_WIDTH, MODEL_WIDTH), jnp.float32) * (2.0 / (NUM_STAGES * HIDDEN_WIDTH)) ** 0.5).astype(jnp.bfloat16)
    mtp_up = (jax.random.normal(key_mup, (MODEL_WIDTH, HIDDEN_WIDTH), jnp.float32) * MODEL_WIDTH ** -0.5).astype(jnp.bfloat16)
    mtp_down = (jax.random.normal(key_mdown, (HIDDEN_WIDTH, MODEL_WIDTH), jnp.float32) * HIDDEN_WIDTH ** -0.5).astype(jnp.bfloat16)
    return {'token_ids': token_ids, 'label_ids': label_ids, 'label2_ids': label2_ids, 'embed_table': embed_table, 'w_up': w_up, 'w_down': w_down, 'mtp_up': mtp_up, 'mtp_down': mtp_down}


def mlp_block(x_in, w_in, w_out):
    pre_act = jnp.dot(x_in, w_in, preferred_element_type=jnp.float32)
    hid_act = jax.nn.gelu(pre_act).astype(jnp.bfloat16)
    out_f = x_in.astype(jnp.float32) + jnp.dot(hid_act, w_out, preferred_element_type=jnp.float32)
    return out_f.astype(jnp.bfloat16)


def block_back(x_in, d_out, w_in, w_out):
    pre_act = jnp.dot(x_in, w_in, preferred_element_type=jnp.float32)
    gelu_out, gelu_back = jax.vjp(jax.nn.gelu, pre_act)
    hid_act = gelu_out.astype(jnp.bfloat16)
    d_hid = jnp.dot(d_out, w_out.T, preferred_element_type=jnp.float32)
    d_pre = gelu_back(d_hid)[0].astype(jnp.bfloat16)
    d_in = d_out.astype(jnp.float32) + jnp.dot(d_pre, w_in.T, preferred_element_type=jnp.float32)
    return d_in, d_pre, hid_act


def rms_fwd(stacked):
    stack_f = stacked.astype(jnp.float32)
    inv_rms = lax.rsqrt(jnp.mean(stack_f * stack_f, axis=-1, keepdims=True) + EPS_NORM)
    return stack_f * inv_rms, inv_rms


def rms_back(normed_f, inv_rms, d_norm):
    return inv_rms * (d_norm - normed_f * jnp.mean(d_norm * normed_f, axis=-1, keepdims=True))


def heads_back(hidden, lab_m, lab2_m, embed_table, mtp_up, mtp_down):
    vocab_size, model_width = embed_table.shape
    logit_scale = model_width ** -0.5
    n_tok = hidden.shape[0]
    g_in = (hidden.astype(jnp.float32) + embed_table[lab_m].astype(jnp.float32)).astype(jnp.bfloat16)
    g_out = mlp_block(g_in, mtp_up, mtp_down)
    stacked = jnp.concatenate([hidden, g_out], axis=0)
    targets = jnp.concatenate([lab_m, lab2_m], axis=0)
    normed_f, inv_rms = rms_fwd(stacked)
    normed = normed_f.astype(jnp.bfloat16)
    logits = jnp.dot(normed, embed_table.T, preferred_element_type=jnp.float32) * logit_scale
    log_norm = jax.nn.logsumexp(logits, axis=-1)
    is_label = targets[:, None] == jnp.arange(vocab_size)[None, :]
    picked = jnp.sum(jnp.where(is_label, logits, 0.0), axis=-1)
    soft_probs = jnp.exp(logits - log_norm[:, None])
    d_logit = (0.5 * logit_scale * (soft_probs - is_label.astype(jnp.float32))).astype(jnp.bfloat16)
    head_grad = jnp.dot(d_logit.T, normed, preferred_element_type=jnp.float32)
    d_norm = jnp.dot(d_logit, embed_table, preferred_element_type=jnp.float32)
    d_stack = rms_back(normed_f, inv_rms, d_norm)
    d_gin, _, _ = block_back(g_in, d_stack[n_tok:].astype(jnp.bfloat16), mtp_up, mtp_down)
    emb_grad = head_grad + jax.ops.segment_sum(d_gin, lab_m, num_segments=vocab_size)
    d_hidden = (d_stack[:n_tok] + d_gin).astype(jnp.bfloat16)
    return 0.5 * jnp.sum(log_norm - picked), emb_grad, d_hidden


def reference(token_ids, label_ids, label2_ids, embed_table, w_up, w_down, mtp_up, mtp_down):
    vocab_size, model_width = embed_table.shape

    def micro_step(loop_state, packed):
        loss_acc, up_acc, down_acc, emb_acc = loop_state
        tok_m, lab_m, lab2_m = packed

        def fwd_layer(x_in, weights):
            return mlp_block(x_in, weights[0], weights[1]), x_in

        hidden, layer_inputs = lax.scan(fwd_layer, embed_table[tok_m], (w_up, w_down))
        loss_m, grad_m, d_hidden = heads_back(hidden, lab_m, lab2_m, embed_table, mtp_up, mtp_down)

        def bwd_layer(d_out, layer_pack):
            x_in, w_in, w_out = layer_pack
            d_in, d_pre, hid_act = block_back(x_in, d_out, w_in, w_out)
            layer_grads = (jnp.dot(x_in.T, d_pre, preferred_element_type=jnp.float32), jnp.dot(hid_act.T, d_out, preferred_element_type=jnp.float32))
            return d_in.astype(jnp.bfloat16), layer_grads

        d_first, (g_up, g_down) = lax.scan(bwd_layer, d_hidden, (layer_inputs, w_up, w_down), reverse=True)
        emb_acc = emb_acc + grad_m + jax.ops.segment_sum(d_first.astype(jnp.float32), tok_m, num_segments=vocab_size)
        return (loss_acc + loss_m, up_acc + g_up, down_acc + g_down, emb_acc), None

    init_state = (jnp.zeros((), jnp.float32), jnp.zeros(w_up.shape, jnp.float32), jnp.zeros(w_down.shape, jnp.float32), jnp.zeros((vocab_size, model_width), jnp.float32))
    (loss_sum, up_sum, down_sum, emb_sum), _ = lax.scan(micro_step, init_state, (token_ids, label_ids, label2_ids))
    mean_loss = (loss_sum / (token_ids.shape[0] * token_ids.shape[1])).reshape(1)
    return mean_loss, up_sum, down_sum, emb_sum
```

```python
import functools
import math

import jax
import jax.numpy as jnp
from jax import lax
from jax.experimental import pallas as pl
from jax.experimental.pallas import tpu as pltpu
from jax.sharding import PartitionSpec as P

EPS_NORM = 1e-6
BF = jnp.bfloat16
F32 = jnp.float32
AXIS = 'stage'
GELU_A = math.sqrt(2.0 / math.pi)
GELU_B = 0.044715
VMEM_MAX = 67000000

VMEM = pl.BlockSpec(memory_space=pltpu.VMEM)
ANY = pl.BlockSpec(memory_space=pl.ANY)
SMEM = pl.BlockSpec(memory_space=pltpu.SMEM)
NN = (((1,), (0,)), ((), ()))
NT = (((1,), (1,)), ((), ()))


def mm(a, b):
    return lax.dot_general(a, b, NN, preferred_element_type=F32)


def mm_t(a, b):
    return lax.dot_general(a, b, NT, preferred_element_type=F32)


def gelu(v):
    return 0.5 * v * (1.0 + jnp.tanh(GELU_A * (v + GELU_B * (v * v * v))))


def gelu_both(v):
    sq = v * v
    t = jnp.tanh(GELU_A * (v + GELU_B * (sq * v)))
    half = 0.5 * (1.0 + t)
    slope = half + (0.5 * v) * (1.0 - t * t) * (GELU_A * (1.0 + (3.0 * GELU_B) * sq))
    return v * half, slope


def dev(d):
    return {AXIS: d}


def greet_all(n_dev):
    me = lax.axis_index(AXIS)
    bar = pltpu.get_barrier_semaphore()
    for d in range(1, n_dev):
        pl.semaphore_signal(bar, inc=1, device_id=dev(lax.rem(me + d, n_dev)), device_id_type=pl.DeviceIdType.MESH)
    pl.semaphore_wait(bar, n_dev - 1)
    return me


def rcopy(src, dst, ssem, rsem, d):
    return pltpu.make_async_remote_copy(src_ref=src, dst_ref=dst, send_sem=ssem, recv_sem=rsem, device_id=dev(d), device_id_type=pl.DeviceIdType.MESH)


def rows(c, size):
    return pl.ds(pl.multiple_of(c * size, size), size)


def mlp_rows(x, wi_ref, wo_ref, tile):
    acc = None
    for f in range(0, wi_ref.shape[1], tile):
        hid = gelu(mm(x, wi_ref[:, f:f + tile])).astype(BF)
        part = mm(hid, wo_ref[f:f + tile, :])
        acc = part if acc is None else acc + part
    return (x.astype(F32) + acc).astype(BF)


def fwd_kernel(S, C, tile, x_ref, wi_ref, wo_ref, xs_ref, h_ref, ob, own_sem, send_sem, recv_sem, h_sem):
    n_rows = xs_ref.shape[0]
    own = x_ref.shape[0]
    n_chunk, per = n_rows // C, own // C
    me = greet_all(S)
    nxt = lax.rem(me + 1, S)

    def own_copy(j):
        c = me * per + j
        return rcopy(x_ref.at[rows(j, C)], xs_ref.at[rows(c, C)], own_sem.at[j], recv_sem.at[c], lax.rem(S - me, S))

    @pl.when(me > 0)
    def _():
        for j in range(per):
            rcopy(x_ref.at[rows(j, C)], xs_ref.at[rows(me * per + j, C)], own_sem.at[j], recv_sem.at[me * per + j], 0).start()

    @pl.when(me == 0)
    def _():
        xs_ref[0:own, :] = x_ref[...]

    def step(c, carry):
        @pl.when((me > 0) | (c >= per))
        def _():
            rcopy(xs_ref.at[rows(c, C)], xs_ref.at[rows(c, C)], send_sem.at[c], recv_sem.at[c], nxt).wait_recv()

        ob[rows(c, C), :] = mlp_rows(xs_ref[rows(c, C), :], wi_ref, wo_ref, tile)
        owner = c // per
        j = lax.rem(c, per)

        @pl.when(me < S - 1)
        def _():
            rcopy(ob.at[rows(c, C)], xs_ref.at[rows(c, C)], send_sem.at[c], recv_sem.at[c], nxt).start()

        @pl.when((me == S - 1) & (owner < S - 1))
        def _():
            rcopy(ob.at[rows(c, C)], h_ref.at[rows(j, C)], send_sem.at[c], h_sem.at[j], owner).start()

        @pl.when((me == S - 1) & (owner == S - 1))
        def _():
            h_ref[rows(j, C), :] = ob[rows(c, C), :]
        return carry

    lax.fori_loop(0, n_chunk, step, 0)

    @pl.when(me > 0)
    def _():
        for j in range(per):
            rcopy(x_ref.at[rows(j, C)], xs_ref.at[rows(me * per + j, C)], own_sem.at[j], recv_sem.at[me * per + j], 0).wait_send()

    def drain(c, carry):
        @pl.when((me < S - 1) | (c < (S - 1) * per))
        def _():
            rcopy(ob.at[rows(c, C)], xs_ref.at[rows(c, C)], send_sem.at[c], recv_sem.at[c], nxt).wait_send()
        return carry

    lax.fori_loop(0, n_chunk, drain, 0)

    @pl.when(me < S - 1)
    def _():
        for j in range(per):
            rcopy(ob.at[rows(j, C)], h_ref.at[rows(j, C)], send_sem.at[j], h_sem.at[j], nxt).wait_recv()


def forward(S, C, tile, x_own, w_in, w_out):
    own, width = x_own.shape
    n_rows = own * S
    n_chunk, per = n_rows // C, own // C
    return pl.pallas_call(
        functools.partial(fwd_kernel, S, C, tile),
        out_shape=(jax.ShapeDtypeStruct((n_rows, width), BF), jax.ShapeDtypeStruct((own, width), BF)),
        in_specs=[VMEM] * 3,
        out_specs=(VMEM, VMEM),
        scratch_shapes=[
            pltpu.VMEM((n_rows, width), BF),
            pltpu.SemaphoreType.DMA((per,)),
            pltpu.SemaphoreType.DMA((n_chunk,)),
            pltpu.SemaphoreType.DMA((n_chunk,)),
            pltpu.SemaphoreType.DMA((per,)),
        ],
        compiler_params=pltpu.CompilerParams(collective_id=0, has_side_effects=True, vmem_limit_bytes=VMEM_MAX),
        cost_estimate=pl.CostEstimate(flops=4 * n_rows * width * w_in.shape[1], bytes_accessed=4 * w_in.size, transcendentals=0),
        name='fwd_pipe',
    )(x_own, w_in, w_out)


def heads_kernel(S, TV, tile, h_ref, e1_ref, e2_ref, tg_ref, wi_ref, wo_ref, emb_ref,
                 nall_ref, lall_ref, dh_ref, dg_ref,
                 ebuf, erem, lrow, gbuf, nf_buf, inv_buf, dn_buf, esem, rsem, nsend, nrecv, lsend, lrecv):
    R, D = h_ref.shape
    V = emb_ref.shape[0]
    n_full = V // TV
    rem = V - n_full * TV
    scale = D ** -0.5
    c2 = scale * math.log2(math.e)
    k = 0.5 * scale
    me = greet_all(S)

    def fetch(i, slot):
        return pltpu.make_async_copy(emb_ref.at[rows(i, TV)], ebuf.at[slot], esem.at[slot])

    fetch(0, 0).start()
    rem_copy = pltpu.make_async_copy(emb_ref.at[pl.ds(n_full * TV, rem)], erem, rsem)
    rem_copy.start()

    hf = h_ref[...].astype(F32)
    g_in = (hf + e1_ref[...].astype(F32)).astype(BF)
    gbuf[...] = g_in
    g_out = mlp_rows(g_in, wi_ref, wo_ref, tile).astype(F32)
    for j, v in enumerate((hf, g_out)):
        inv = lax.rsqrt(jnp.mean(v * v, axis=-1, keepdims=True) + EPS_NORM)
        nf = v * inv
        nf_buf[j * R:(j + 1) * R, :] = nf
        inv_buf[j * R:(j + 1) * R, :] = jnp.broadcast_to(inv, (R, 128))
        nall_ref[me, j * R:(j + 1) * R, :] = nf.astype(BF)

    def ncopy(d):
        return rcopy(nall_ref.at[me], nall_ref.at[me], nsend.at[d], nrecv.at[d], lax.rem(me + d, S))

    def lcopy(d):
        return rcopy(lall_ref.at[me], lall_ref.at[me], lsend.at[d], lrecv.at[d], lax.rem(me + d, S))

    for d in range(1, S):
        ncopy(d).start()

    def fold(et, mx, sm):
        lt = mm_t(et, nall_ref[me])
        grp = lt.reshape(et.shape[0] // 8, 8, 2 * R)
        new = jnp.maximum(mx, jnp.max(grp, axis=0))
        sm = sm * jnp.exp2((mx - new) * c2) + jnp.sum(jnp.exp2((grp - new[None]) * c2), axis=0)
        return new, sm

    def p1(i, carry):
        slot = lax.rem(i, 2)
        fetch(i, slot).wait()

        fetch(lax.rem(i + 1, n_full), 1 - slot).start()
        return fold(ebuf[slot], *carry)

    mx, sm = lax.fori_loop(0, n_full, p1, (jnp.full((8, 2 * R), -jnp.inf, F32), jnp.zeros((8, 2 * R), F32)))
    rem_copy.wait()
    mx, sm = fold(erem[...], mx, sm)
    top = jnp.max(mx, axis=0, keepdims=True)
    tot = jnp.sum(sm * jnp.exp2((mx - top) * c2), axis=0, keepdims=True)
    lse2 = top * c2 + jnp.log(tot) * math.log2(math.e)
    lrow[...] = jnp.broadcast_to(lse2, (128, 2 * R))
    lcol = jnp.transpose(lrow[...])[:, 0:1]
    nrm = nall_ref[me].astype(F32)
    pick = jnp.concatenate([
        jnp.sum(nrm[:R] * e1_ref[...].astype(F32), axis=-1, keepdims=True),
        jnp.sum(nrm[R:] * e2_ref[...].astype(F32), axis=-1, keepdims=True)], axis=0) * scale
    nll = jnp.sum(lcol * math.log(2.0) - pick, axis=0, keepdims=True)
    lall_ref[me] = jnp.where(lax.broadcasted_iota(jnp.int32, (8, 2 * R), 0) == 0, jnp.broadcast_to(lse2, (8, 2 * R)), jnp.broadcast_to(nll, (8, 2 * R)))
    for d in range(1, S):
        lcopy(d).start()

    shift = lcol - math.log2(k)
    tg = tg_ref[...]
    dn_buf[...] = jnp.zeros_like(dn_buf)

    def back(et, base):
        n = et.shape[0]
        logit = mm_t(nall_ref[me], et)
        q = jnp.exp2(logit * c2 - shift)
        hit = lax.broadcasted_iota(jnp.int32, (2 * R, n), 1) == tg - base
        dl = jnp.where(hit, q - k, q).astype(BF)
        dn_buf[...] += mm(dl, et)

    first = n_full % 2

    def p2(i, carry):
        slot = lax.rem(i + first, 2)
        fetch(i, slot).wait()

        @pl.when(i + 1 < n_full)
        def _():
            fetch(i + 1, 1 - slot).start()
        back(ebuf[slot], i * TV)
        return carry

    lax.fori_loop(0, n_full, p2, 0)
    back(erem[...], n_full * TV)

    dn = dn_buf[...]
    nf = nf_buf[...]
    ds = inv_buf[:, 0:1] * (dn - nf * jnp.mean(dn * nf, axis=-1, keepdims=True))
    dout = ds[R:].astype(BF)
    g_in = gbuf[...]
    acc = dout.astype(F32)
    for f in range(0, wi_ref.shape[1], tile):
        w1 = wi_ref[:, f:f + tile]
        _, slope = gelu_both(mm(g_in, w1))
        dpre = (mm_t(dout, wo_ref[f:f + tile, :]) * slope).astype(BF)
        acc += mm_t(dpre, w1)
    dg_ref[...] = acc
    dh_ref[...] = (ds[:R] + acc).astype(BF)

    for d in range(1, S):
        ncopy(d).wait_send()
        lcopy(d).wait_send()
        rcopy(nall_ref.at[me], nall_ref.at[lax.rem(me + S - d, S)], nsend.at[d], nrecv.at[d], lax.rem(me + d, S)).wait_recv()
        rcopy(lall_ref.at[me], lall_ref.at[lax.rem(me + S - d, S)], lsend.at[d], lrecv.at[d], lax.rem(me + d, S)).wait_recv()


def heads(S, TV, tile, h_own, e1, e2, tg, mtp_up, mtp_down, emb):
    R, D = h_own.shape
    V = emb.shape[0]
    rem = V % TV
    return pl.pallas_call(
        functools.partial(heads_kernel, S, TV, tile),
        out_shape=(jax.ShapeDtypeStruct((S, 2 * R, D), BF), jax.ShapeDtypeStruct((S, 8, 2 * R), F32),
                   jax.ShapeDtypeStruct((R, D), BF), jax.ShapeDtypeStruct((R, D), F32)),
        in_specs=[VMEM] * 6 + [ANY],
        out_specs=(VMEM,) * 4,
        scratch_shapes=[
            pltpu.VMEM((2, TV, D), BF),
            pltpu.VMEM((rem, D), BF),
            pltpu.VMEM((128, 2 * R), F32),
            pltpu.VMEM((R, D), BF),
            pltpu.VMEM((2 * R, D), F32),
            pltpu.VMEM((2 * R, 128), F32),
            pltpu.VMEM((2 * R, D), F32),
            pltpu.SemaphoreType.DMA((2,)),
            pltpu.SemaphoreType.DMA,
            pltpu.SemaphoreType.DMA((S,)),
            pltpu.SemaphoreType.DMA((S,)),
            pltpu.SemaphoreType.DMA((S,)),
            pltpu.SemaphoreType.DMA((S,)),
        ],
        compiler_params=pltpu.CompilerParams(collective_id=1, has_side_effects=True, vmem_limit_bytes=VMEM_MAX),
        cost_estimate=pl.CostEstimate(flops=12 * R * D * V, bytes_accessed=4 * V * D, transcendentals=4 * R * V),
        name='heads',
    )(h_own, e1, e2, tg, mtp_up, mtp_down, emb)


def bwd_kernel(S, C, tile, dh_ref, xs_ref, wi_ref, wo_ref, ds_ref, dpre_ref, hid_ref, dx_ref,
               ob, pbuf, hbuf, own_sem, send_sem, recv_sem, psem, hsem, bsend, brecv):
    n_rows = xs_ref.shape[0]
    own = dh_ref.shape[0]
    F = wi_ref.shape[1]
    n_chunk, per = n_rows // C, own // C
    me = greet_all(S)
    last = S - 1
    prv = lax.rem(me + S - 1, S)
    half = S // 2

    @pl.when(me < last)
    def _():
        for j in range(per):
            rcopy(dh_ref.at[rows(j, C)], ds_ref.at[rows(me * per + j, C)], own_sem.at[j], recv_sem.at[me * per + j], last).start()

    @pl.when(me == last)
    def _():
        ds_ref[last * own:, :] = dh_ref[...]

    def spread(c, stop):
        def to(i, d):
            cp = rcopy(dx_ref.at[rows(c, C)], dx_ref.at[rows(c, C)], bsend.at[i, c], brecv.at[c], d)
            cp.wait_send() if stop else cp.start()

        @pl.when(lax.rem(me, 2) == 0)
        def _():
            to(0, me + 1)

        @pl.when((lax.rem(me, 2) == 0) & (me < half))
        def _():
            to(1, me + 2)

        @pl.when((me == 0) | ((lax.rem(me, 2) == 0) & (me > half + 2)))
        def _():
            to(2, lax.rem(me + S - 2, S))

    def out_copies(c):
        slot = lax.rem(c, 2)
        return (pltpu.make_async_copy(pbuf.at[slot], dpre_ref.at[rows(c, C)], psem.at[slot]),
                pltpu.make_async_copy(hbuf.at[slot], hid_ref.at[rows(c, C)], hsem.at[slot]))

    def step(c, carry):
        slot = lax.rem(c, 2)

        @pl.when(c >= 2)
        def _():
            for cp in out_copies(c - 2):
                cp.wait()

        @pl.when((me < last) | (c < last * per))
        def _():
            rcopy(ds_ref.at[rows(c, C)], ds_ref.at[rows(c, C)], send_sem.at[c], recv_sem.at[c], prv).wait_recv()

        x = xs_ref[rows(c, C), :]
        dout = ds_ref[rows(c, C), :]
        acc = dout.astype(F32)
        for f in range(0, F, tile):
            w1 = wi_ref[:, f:f + tile]
            hid, slope = gelu_both(mm(x, w1))
            dpre = (mm_t(dout, wo_ref[f:f + tile, :]) * slope).astype(BF)
            hbuf[slot, :, f:f + tile] = hid.astype(BF)
            pbuf[slot, :, f:f + tile] = dpre
            acc += mm_t(dpre, w1)
        res = acc.astype(BF)

        @pl.when(me > 0)
        def _():
            ob[rows(c, C), :] = res
            rcopy(ob.at[rows(c, C)], ds_ref.at[rows(c, C)], send_sem.at[c], recv_sem.at[c], prv).start()

        @pl.when(me == 0)
        def _():
            dx_ref[rows(c, C), :] = res
            spread(c, False)

        for cp in out_copies(c):
            cp.start()
        return carry

    lax.fori_loop(0, n_chunk, step, 0)

    for c in (n_chunk - 2, n_chunk - 1):
        for cp in out_copies(c):
            cp.wait()

    @pl.when(me < last)
    def _():
        for j in range(per):
            rcopy(dh_ref.at[rows(j, C)], ds_ref.at[rows(me * per + j, C)], own_sem.at[j], recv_sem.at[me * per + j], last).wait_send()

    def drain(c, carry):
        @pl.when(me > 0)
        def _():
            rcopy(ob.at[rows(c, C)], ds_ref.at[rows(c, C)], send_sem.at[c], recv_sem.at[c], prv).wait_send()
            rcopy(dx_ref.at[rows(c, C)], dx_ref.at[rows(c, C)], bsend.at[0, c], brecv.at[c], prv).wait_recv()
            spread(c, False)
        return carry

    lax.fori_loop(0, n_chunk, drain, 0)

    def settle(c, carry):
        spread(c, True)
        return carry

    lax.fori_loop(0, n_chunk, settle, 0)


def backward(S, C, tile, dh, xs, w_in, w_out):
    own, D = dh.shape
    n_rows = xs.shape[0]
    F = w_in.shape[1]
    n_chunk, per = n_rows // C, own // C
    return pl.pallas_call(
        functools.partial(bwd_kernel, S, C, tile),
        out_shape=(jax.ShapeDtypeStruct((n_rows, D), BF), jax.ShapeDtypeStruct((n_rows, F), BF),
                   jax.ShapeDtypeStruct((n_rows, F), BF), jax.ShapeDtypeStruct((n_rows, D), BF)),
        in_specs=[VMEM] * 4,
        out_specs=(VMEM, ANY, ANY, VMEM),
        scratch_shapes=[
            pltpu.VMEM((n_rows, D), BF),
            pltpu.VMEM((2, C, F), BF),
            pltpu.VMEM((2, C, F), BF),
            pltpu.SemaphoreType.DMA((per,)),
            pltpu.SemaphoreType.DMA((n_chunk,)),
            pltpu.SemaphoreType.DMA((n_chunk,)),
            pltpu.SemaphoreType.DMA((2,)),
            pltpu.SemaphoreType.DMA((2,)),
            pltpu.SemaphoreType.DMA((3, n_chunk)),
            pltpu.SemaphoreType.DMA((n_chunk,)),
        ],
        compiler_params=pltpu.CompilerParams(collective_id=2, has_side_effects=True, vmem_limit_bytes=VMEM_MAX),
        cost_estimate=pl.CostEstimate(flops=12 * n_rows * D * F, bytes_accessed=8 * n_rows * F, transcendentals=0),
        name='bwd_pipe',
    )(dh, xs, w_in, w_out)


def head_tile(et, base, nall_ref, lse_ref, tgt_ref, block):
    D = et.shape[1]
    c2 = D ** -0.5 * math.log2(math.e)
    k = 0.5 * D ** -0.5
    acc = None
    for j in range(0, nall_ref.shape[0], block):
        nb = nall_ref[j:j + block, :]
        q = jnp.exp2(mm_t(et, nb) * c2 - (lse_ref[:, j:j + block] - math.log2(k)))
        hit = lax.broadcasted_iota(jnp.int32, q.shape, 0) == tgt_ref[:, j:j + block] - base
        part = mm(jnp.where(hit, q - k, q).astype(BF), nb)
        acc = part if acc is None else acc + part
    return acc


def shard_kernel(block, off_ref, e_ref, nall_ref, lse_ref, tgt_ref, o_ref):
    tv = e_ref.shape[0]
    base = (off_ref[0] + pl.program_id(0)) * tv
    o_ref[...] = head_tile(e_ref[...], base, nall_ref, lse_ref, tgt_ref, block)


def head_shard(tv, n_tile, block, off, emb, nall, lse, tgt):
    D = emb.shape[1]
    return pl.pallas_call(
        functools.partial(shard_kernel, block),
        out_shape=jax.ShapeDtypeStruct((n_tile * tv, D), F32),
        grid_spec=pltpu.PrefetchScalarGridSpec(
            num_scalar_prefetch=1, grid=(n_tile,),
            in_specs=[pl.BlockSpec((tv, D), lambda i, o: (o[0] + i, 0)), VMEM, VMEM, VMEM],
            out_specs=pl.BlockSpec((tv, D), lambda i, o: (i, 0))),
        compiler_params=pltpu.CompilerParams(vmem_limit_bytes=VMEM_MAX),
        cost_estimate=pl.CostEstimate(flops=4 * n_tile * tv * D * nall.shape[0], bytes_accessed=6 * n_tile * tv * D, transcendentals=n_tile * tv * nall.shape[0]),
        name='head_shard',
    )(off, emb, nall, lse, tgt)


def add_rows(o_ref, base, lo, hi, ids_ref, mats):
    tv = o_ref.shape[0]

    def body(b, carry):
        hit = lax.broadcasted_iota(jnp.int32, (tv, 128), 0) == ids_ref[pl.ds(b, 1), :] - base
        oh = jnp.where(hit, 1.0, 0.0).astype(BF)
        part = None
        for m in mats:
            p = mm(oh, m[rows(b, 128), :])
            part = p if part is None else part + p
        o_ref[...] += part
        return carry

    lax.fori_loop(lo, hi, body, 0)


def local_kernel(block, tile0, lim_ref, e_ref, nall_ref, lse_ref, tgt_ref, ids_ref, dx_ref, lids_ref, g0_ref, g1_ref, g2_ref, o_ref):
    tv = e_ref.shape[0]
    t = pl.program_id(0) + tile0
    base = t * tv
    o_ref[...] = head_tile(e_ref[...], base, nall_ref, lse_ref, tgt_ref, block)
    add_rows(o_ref, base, lim_ref[0, t], lim_ref[1, t], ids_ref, (dx_ref,))
    add_rows(o_ref, base, lim_ref[2, t], lim_ref[3, t], lids_ref, (g0_ref, g1_ref, g2_ref))


def local_part(tv, tile0, block, lim, emb, nall, lse, tgt, ids, dx, lids, g3):
    V, D = emb.shape
    n_tile = pl.cdiv(V, tv) - tile0
    return pl.pallas_call(
        functools.partial(local_kernel, block, tile0),
        out_shape=jax.ShapeDtypeStruct((V, D), F32),
        grid=(n_tile,),
        in_specs=[SMEM, pl.BlockSpec((tv, D), lambda i: (i + tile0, 0))] + [VMEM] * 9,
        out_specs=pl.BlockSpec((tv, D), lambda i: (i + tile0, 0)),
        compiler_params=pltpu.CompilerParams(vmem_limit_bytes=VMEM_MAX),
        cost_estimate=pl.CostEstimate(flops=4 * n_tile * tv * D * nall.shape[0], bytes_accessed=6 * n_tile * tv * D, transcendentals=n_tile * tv * nall.shape[0]),
        name='head_local',
    )(lim, emb, nall, lse, tgt, ids, dx, lids, *g3)


def sweep_kernel(lim_ref, full_ref, a_ref, ids_ref, dx_ref, lids_ref, g0_ref, g1_ref, g2_ref, o_ref):
    t = pl.program_id(0)
    base = t * o_ref.shape[0]
    o_ref[...] = a_ref[...]
    add_rows(o_ref, base, lim_ref[0, t], lim_ref[1, t], ids_ref, (dx_ref,))
    add_rows(o_ref, base, lim_ref[2, t], lim_ref[3, t], lids_ref, (g0_ref, g1_ref, g2_ref))


def sweep(tv, lim, full, gathered, ids, dx, lids, g3):
    n, D = gathered.shape
    return pl.pallas_call(
        sweep_kernel,
        out_shape=jax.ShapeDtypeStruct(full.shape, F32),
        grid=(n // tv,),
        in_specs=[SMEM, ANY, pl.BlockSpec((tv, D), lambda i: (i, 0))] + [VMEM] * 6,
        out_specs=pl.BlockSpec((tv, D), lambda i: (i, 0)),
        input_output_aliases={1: 0},
        compiler_params=pltpu.CompilerParams(vmem_limit_bytes=VMEM_MAX),
        cost_estimate=pl.CostEstimate(flops=n * D, bytes_accessed=8 * n * D, transcendentals=0),
        name='sweep',
    )(lim, full, gathered, ids, dx, lids, *g3)


def limits(sorted_ids, tv, n_tile):
    edge = jnp.arange(n_tile + 1, dtype=jnp.int32) * tv
    below = jnp.sum((sorted_ids[None, :] < edge[:, None]).astype(jnp.int32), axis=1)
    lo, hi = below[:-1], below[1:]
    return lo // 128, jnp.where(hi > lo, (hi + 127) // 128, lo // 128)


SHARED = 0.64
TILE_V = 512


def solution(mesh):
    S = mesh.shape[AXIS]

    def per_device(token_ids, label_ids, label2_ids, embed_table, w_up, w_down, mtp_up, mtp_down):
        V, D = embed_table.shape
        N = token_ids.size
        R = N // S
        me = lax.axis_index(AXIS)
        w_in, w_out = w_up[0], w_down[0]

        tok, lab, lab2 = lax.sort((token_ids.reshape(N), label_ids.reshape(N), label2_ids.reshape(N)), num_keys=1)
        lab_sorted, lab_perm = lax.sort((lab, lax.iota(jnp.int32, N)), num_keys=1)

        def own(v):
            return lax.dynamic_slice_in_dim(v, me * R, R)

        picked = embed_table[jnp.concatenate([own(tok), own(lab), own(lab2)])]
        x_own, e1, e2 = picked[:R], picked[R:2 * R], picked[2 * R:]
        xs, h_own = forward(S, R, 1024, x_own, w_in, w_out)
        tg = jnp.concatenate([own(lab), own(lab2)]).reshape(2 * R, 1)
        nall, lall, dh, dg = heads(S, 1024, 1024, h_own, e1, e2, tg, mtp_up, mtp_down, embed_table)
        nall = nall.reshape(2 * N, D)
        lse = lall[:, 0, :].reshape(1, 2 * N)
        loss = (0.5 * jnp.sum(lall[:, 1, 0]) / N).reshape(1)
        tgt = jnp.stack([lab.reshape(S, R), lab2.reshape(S, R)], axis=1).reshape(1, 2 * N)

        dg_all = lax.all_gather(dg, AXIS, axis=0, tiled=True)
        n_tile = pl.cdiv(V, TILE_V)
        shard_tiles = int(V * SHARED) // (S * TILE_V)
        n_shared = shard_tiles * S
        mine = head_shard(TILE_V, shard_tiles, 1024, (me * shard_tiles).reshape(1), embed_table, nall, lse, tgt)
        gathered = lax.all_gather(mine, AXIS, axis=0, tiled=True)

        dsv, dpre, hid, dx = backward(S, R, 1024, dh, xs, w_in, w_out)
        g_up = lax.dot_general(xs, dpre, (((0,), (0,)), ((), ())), preferred_element_type=F32)
        g_down = lax.dot_general(hid, dsv, (((0,), (0,)), ((), ())), preferred_element_type=F32)

        dg_rows = dg_all[lab_perm]
        g0 = dg_rows.astype(BF)
        r1 = dg_rows - lax.reduce_precision(dg_rows, 8, 7)
        g1 = r1.astype(BF)
        g2 = (r1 - lax.reduce_precision(r1, 8, 7)).astype(BF)
        lim = jnp.stack(limits(tok, TILE_V, n_tile) + limits(lab_sorted, TILE_V, n_tile))
        ids = tok.reshape(N // 128, 128)
        lids = lab_sorted.reshape(N // 128, 128)
        full = local_part(TILE_V, n_shared, 1024, lim, embed_table, nall, lse, tgt, ids, dx, lids, (g0, g1, g2))
        grad_emb = sweep(TILE_V, lim, full, gathered, ids, dx, lids, (g0, g1, g2))
        return loss, g_up[None], g_down[None], grad_emb

    in_specs = (P('dp', None), P('dp', None), P('dp', None), P(None, None), P('stage', None, None), P('stage', None, None), P(None, None), P(None, None))
    out_specs = (P('dp'), P(('dp', 'stage'), None, None), P(('dp', 'stage'), None, None), P('dp', None))
    return jax.shard_map(per_device, mesh=mesh, in_specs=in_specs, out_specs=out_specs, check_vma=False)
```

```python
import functools
import math

import jax
import jax.numpy as jnp
from jax import lax
from jax.experimental import pallas as pl
from jax.experimental.pallas import tpu as pltpu
from jax.sharding import PartitionSpec as P


EPS_NORM = 1e-6
BF = jnp.bfloat16
F32 = jnp.float32
AXIS = 'stage'
GELU_A = math.sqrt(2.0 / math.pi)
GELU_B = 0.044715
VMEM_MAX = 67000000
DEPTH = 4

VMEM = pl.BlockSpec(memory_space=pltpu.VMEM)
ANY = pl.BlockSpec(memory_space=pl.ANY)
SMEM = pl.BlockSpec(memory_space=pltpu.SMEM)
NN = (((1,), (0,)), ((), ()))
NT = (((1,), (1,)), ((), ()))


def cost(work, elems):
    return pl.CostEstimate(flops=8 * work, bytes_accessed=8 * elems, transcendentals=0)


def mm(a, b):
    return lax.dot_general(a, b, NN, preferred_element_type=F32)


def mm_t(a, b):
    return lax.dot_general(a, b, NT, preferred_element_type=F32)


def gelu(v):
    return 0.5 * v * (1.0 + jnp.tanh(GELU_A * (v + GELU_B * (v * v * v))))


def gelu_both(v):
    sq = v * v
    t = jnp.tanh(GELU_A * (v + GELU_B * (sq * v)))
    half = 0.5 * (1.0 + t)
    slope = half + (0.5 * v) * (1.0 - t * t) * (GELU_A * (1.0 + (3.0 * GELU_B) * sq))
    return v * half, slope


def dev(d):
    return {AXIS: d}


def greet_all(n_dev):
    me = lax.axis_index(AXIS)
    bar = pltpu.get_barrier_semaphore()
    for d in range(1, n_dev):
        pl.semaphore_signal(bar, inc=1, device_id=dev(lax.rem(me + d, n_dev)), device_id_type=pl.DeviceIdType.MESH)
    pl.semaphore_wait(bar, n_dev - 1)
    return me


def rcopy(src, dst, ssem, rsem, d):
    return pltpu.make_async_remote_copy(src_ref=src, dst_ref=dst, send_sem=ssem, recv_sem=rsem, device_id=dev(d), device_id_type=pl.DeviceIdType.MESH)


def rows(c, size):
    return pl.ds(pl.multiple_of(c * size, size), size)


def mlp_rows(x, wi_ref, wo_ref, tile):
    acc = None
    for f in range(0, wi_ref.shape[1], tile):
        hid = gelu(mm(x, wi_ref[:, f:f + tile])).astype(BF)
        part = mm(hid, wo_ref[f:f + tile, :])
        acc = part if acc is None else acc + part
    return (x.astype(F32) + acc).astype(BF)


def fwd_kernel(S, C, tile, x_ref, wi_ref, wo_ref, xs_ref, h_ref, wit_ref, wot_ref, ob, own_sem, send_sem, recv_sem, h_sem):
    n_rows = xs_ref.shape[0]
    own = x_ref.shape[0]
    n_chunk, per = n_rows // C, own // C
    me = greet_all(S)
    nxt = lax.rem(me + 1, S)

    def flip(f, carry):
        wit_ref[rows(f, 512), :] = jnp.transpose(wi_ref[:, rows(f, 512)])
        wot_ref[:, rows(f, 512)] = jnp.transpose(wo_ref[rows(f, 512), :])
        return carry

    early = me >= S // 2

    @pl.when(me > 0)
    def _():
        for j in range(per):
            rcopy(x_ref.at[rows(j, C)], xs_ref.at[rows(me * per + j, C)], own_sem.at[j], recv_sem.at[me * per + j], 0).start()

    @pl.when(me == 0)
    def _():
        xs_ref[0:own, :] = x_ref[...]

    lax.fori_loop(0, jnp.where(early, wi_ref.shape[1] // 512, 0), flip, 0)

    def step(c, carry):
        @pl.when((me > 0) | (c >= per))
        def _():
            rcopy(xs_ref.at[rows(c, C)], xs_ref.at[rows(c, C)], send_sem.at[c], recv_sem.at[c], nxt).wait_recv()

        ob[rows(c, C), :] = mlp_rows(xs_ref[rows(c, C), :], wi_ref, wo_ref, tile)
        owner = c // per
        j = lax.rem(c, per)

        @pl.when(me < S - 1)
        def _():
            rcopy(ob.at[rows(c, C)], xs_ref.at[rows(c, C)], send_sem.at[c], recv_sem.at[c], nxt).start()

        @pl.when((me == S - 1) & (owner < S - 1))
        def _():
            rcopy(ob.at[rows(c, C)], h_ref.at[rows(j, C)], send_sem.at[c], h_sem.at[j], owner).start()

        @pl.when((me == S - 1) & (owner == S - 1))
        def _():
            h_ref[rows(j, C), :] = ob[rows(c, C), :]

        return carry

    lax.fori_loop(0, n_chunk, step, 0)

    @pl.when(me > 0)
    def _():
        for j in range(per):
            rcopy(x_ref.at[rows(j, C)], xs_ref.at[rows(me * per + j, C)], own_sem.at[j], recv_sem.at[me * per + j], 0).wait_send()

    def drain(c, carry):
        @pl.when((me < S - 1) | (c < (S - 1) * per))
        def _():
            rcopy(ob.at[rows(c, C)], xs_ref.at[rows(c, C)], send_sem.at[c], recv_sem.at[c], nxt).wait_send()

        return carry

    lax.fori_loop(0, jnp.where(early, 0, wi_ref.shape[1] // 512), flip, 0)
    lax.fori_loop(0, n_chunk, drain, 0)

    @pl.when(me < S - 1)
    def _():
        for j in range(per):
            rcopy(ob.at[rows(j, C)], h_ref.at[rows(j, C)], send_sem.at[j], h_sem.at[j], nxt).wait_recv()


def forward(S, C, tile, x_own, w_in, w_out):
    own, width = x_own.shape
    n_rows = own * S
    n_chunk, per = n_rows // C, own // C
    return pl.pallas_call(
        functools.partial(fwd_kernel, S, C, tile),
        out_shape=(jax.ShapeDtypeStruct((n_rows, width), BF), jax.ShapeDtypeStruct((own, width), BF),
                   jax.ShapeDtypeStruct(w_out.shape, BF), jax.ShapeDtypeStruct(w_in.shape, BF)),
        in_specs=[VMEM] * 3,
        out_specs=(VMEM,) * 4,
        scratch_shapes=[
            pltpu.VMEM((n_rows, width), BF),
            pltpu.SemaphoreType.DMA((per,)),
            pltpu.SemaphoreType.DMA((n_chunk,)),
            pltpu.SemaphoreType.DMA((n_chunk,)),
            pltpu.SemaphoreType.DMA((per,)),
        ],
        compiler_params=pltpu.CompilerParams(collective_id=0, has_side_effects=True, vmem_limit_bytes=VMEM_MAX),
        cost_estimate=cost(n_rows * w_in.size, w_in.size),
        name='fwd_pipe',
    )(x_own, w_in, w_out)


def stream(emb_ref, ebuf, esem, TV):
    def fetch(i):
        slot = lax.rem(i, ebuf.shape[0])
        return pltpu.make_async_copy(emb_ref.at[rows(i, TV)], ebuf.at[slot], esem.at[slot])

    return fetch


def staged(n_full, first, stage, last):
    first()

    def pair(j, carry):
        carry = stage(2 * j + 1, 1, 0, carry)
        return stage(2 * j + 2, 0, 1, carry)

    return lambda carry: tail(n_full, stage, last, lax.fori_loop(0, (n_full - 1) // 2, pair, carry))


def tail(n_full, stage, last, carry):
    if (n_full - 1) % 2:
        carry = stage(n_full - 1, 1, 0, carry)
    return last((n_full - 1) % 2, carry)


def lse_kernel(S, TV, tile, h_ref, e1_ref, e2_ref, wi_ref, wo_ref, emb_ref,
               nall_ref, lall_ref, st_ref, lcol_ref,
               ebuf, erem, la, lb, lrow, esem, rsem, nsend, nrecv, lsend, lrecv):
    R, D = h_ref.shape
    V = emb_ref.shape[0]
    n_full = V // TV
    rem = V - n_full * TV
    scale = D ** -0.5
    c2 = scale * math.log2(math.e)
    me = greet_all(S)
    fetch = stream(emb_ref, ebuf, esem, TV)
    for i in range(DEPTH):
        fetch(i).start()
    rem_copy = pltpu.make_async_copy(emb_ref.at[pl.ds(n_full * TV, rem)], erem, rsem)
    rem_copy.start()

    hf = h_ref[...].astype(F32)
    st_ref[0:R, :] = h_ref[...]
    g_in = (hf + e1_ref[...].astype(F32)).astype(BF)
    acc_ref = la.at[pl.ds(0, R)]
    acc_ref[...] = jnp.zeros((R, D), F32)

    def mtp(f, carry):
        acc_ref[...] += mm(gelu(mm(g_in, wi_ref[:, rows(f, tile)])).astype(BF), wo_ref[rows(f, tile), :])
        return carry

    lax.fori_loop(0, wi_ref.shape[1] // tile, mtp, 0)
    g_out = (g_in.astype(F32) + acc_ref[...]).astype(BF)
    st_ref[R:, :] = g_out
    for j, v in enumerate((hf, g_out.astype(F32))):
        inv = lax.rsqrt(jnp.mean(v * v, axis=-1, keepdims=True) + EPS_NORM)
        nall_ref[me, j * R:(j + 1) * R, :] = (v * inv).astype(BF)

    sib = me + 1 - 2 * lax.rem(me, 2)

    def block(b, ssem, d):
        return rcopy(nall_ref.at[b], nall_ref.at[b], ssem, nrecv.at[b], d)

    def peer(d):
        return lax.rem(me + 2 * d, S)

    def lcopy(d):
        return rcopy(lall_ref.at[me], lall_ref.at[me], lsend.at[d], lrecv.at[d], lax.rem(me + d, S))

    for d in range(1, S // 2):
        block(me, nsend.at[d], peer(d)).start()
    block(me, nsend.at[0], sib).start()

    bufs = (la, lb)

    def fold(lt, mx, sm):
        grp = lt.reshape(lt.shape[0] // 8, 8, 2 * R)
        new = jnp.maximum(mx, jnp.max(grp, axis=0))
        sm = sm * jnp.exp2((mx - new) * c2) + jnp.sum(jnp.exp2((grp - new[None]) * c2), axis=0)
        return new, sm

    def first():
        fetch(0).wait()
        la[...] = mm_t(ebuf[0], nall_ref[me])

    def stage(i, w, r, carry):
        fetch(i).wait()

        @pl.when(i + DEPTH - 1 < n_full)
        def _():
            fetch(i + DEPTH - 1).start()

        bufs[w][...] = mm_t(ebuf[lax.rem(i, ebuf.shape[0])], nall_ref[me])
        return fold(bufs[r][...], *carry)

    def last(r, carry):
        return fold(bufs[r][...], *carry)

    mx, sm = staged(n_full, first, stage, last)((jnp.full((8, 2 * R), -jnp.inf, F32), jnp.zeros((8, 2 * R), F32)))
    for d in range(1, S // 2):
        block(peer(d), nsend.at[S // 2 + d], sib).wait_recv()
        block(peer(d), nsend.at[S // 2 + d], sib).start()
    rem_copy.wait()
    mx, sm = fold(mm_t(erem[...], nall_ref[me]), mx, sm)
    top = jnp.max(mx, axis=0, keepdims=True)
    tot = jnp.sum(sm * jnp.exp2((mx - top) * c2), axis=0, keepdims=True)
    lse2 = top * c2 + jnp.log(tot) * math.log2(math.e)
    lrow[...] = jnp.broadcast_to(lse2, (128, 2 * R))
    lcol_ref[...] = jnp.transpose(lrow[...])
    nrm = nall_ref[me].astype(F32)
    pick = jnp.concatenate([
        jnp.sum(nrm[:R] * e1_ref[...].astype(F32), axis=-1, keepdims=True),
        jnp.sum(nrm[R:] * e2_ref[...].astype(F32), axis=-1, keepdims=True)], axis=0) * scale
    nll = jnp.sum(lcol_ref[:, 0:1] * math.log(2.0) - pick, axis=0, keepdims=True)
    lall_ref[me] = jnp.where(lax.broadcasted_iota(jnp.int32, (8, 2 * R), 0) == 0, jnp.broadcast_to(lse2, (8, 2 * R)), jnp.broadcast_to(nll, (8, 2 * R)))
    for d in range(1, S):
        lcopy(d).start()
    for d in range(1, S // 2):
        block(me, nsend.at[d], peer(d)).wait_send()
        block(peer(d), nsend.at[S // 2 + d], sib).wait_send()
        block(lax.rem(sib + 2 * d, S), nsend.at[d], sib).wait_recv()
    block(me, nsend.at[0], sib).wait_send()
    block(sib, nsend.at[0], sib).wait_recv()
    for d in range(1, S):
        lcopy(d).wait_send()
        src = lax.rem(me + S - d, S)
        rcopy(lall_ref.at[me], lall_ref.at[src], lsend.at[d], lrecv.at[d], lax.rem(me + d, S)).wait_recv()


def lse_phase(S, TV, tile, h_own, e1, e2, mtp_up, mtp_down, emb):
    R, D = h_own.shape
    V = emb.shape[0]
    return pl.pallas_call(
        functools.partial(lse_kernel, S, TV, tile),
        out_shape=(jax.ShapeDtypeStruct((S, 2 * R, D), BF), jax.ShapeDtypeStruct((S, 8, 2 * R), F32),
                   jax.ShapeDtypeStruct((2 * R, D), BF), jax.ShapeDtypeStruct((2 * R, 128), F32)),
        in_specs=[VMEM] * 5 + [ANY],
        out_specs=(VMEM,) * 4,
        scratch_shapes=[
            pltpu.VMEM((DEPTH, TV, D), BF),
            pltpu.VMEM((V % TV, D), BF),
            pltpu.VMEM((TV, 2 * R), F32),
            pltpu.VMEM((TV, 2 * R), F32),
            pltpu.VMEM((128, 2 * R), F32),
            pltpu.SemaphoreType.DMA((DEPTH,)),
            pltpu.SemaphoreType.DMA,
            pltpu.SemaphoreType.DMA((S,)),
            pltpu.SemaphoreType.DMA((S,)),
            pltpu.SemaphoreType.DMA((S,)),
            pltpu.SemaphoreType.DMA((S,)),
        ],
        compiler_params=pltpu.CompilerParams(collective_id=1, has_side_effects=True, vmem_limit_bytes=VMEM_MAX),
        cost_estimate=cost(R * D * V, V * D),
        name='heads_lse',
    )(h_own, e1, e2, mtp_up, mtp_down, emb)


def grad_kernel(TV, tile, st_ref, e1_ref, tg_ref, lcol_ref, wi_ref, wo_ref, emb_ref, after_ref,
                dh_ref, dg_ref, ebuf, erem, la, lb, nb, dn_buf, esem, rsem):
    R, D = e1_ref.shape
    V = emb_ref.shape[0]
    n_full = V // TV
    rem = V - n_full * TV
    scale = D ** -0.5
    c2 = scale * math.log2(math.e)
    k = 0.5 * scale
    fetch = stream(emb_ref, ebuf, esem, TV)
    for i in range(DEPTH):
        fetch(i).start()
    rem_copy = pltpu.make_async_copy(emb_ref.at[pl.ds(n_full * TV, rem)], erem, rsem)
    rem_copy.start()
    stf = st_ref[...].astype(F32)
    inv = lax.rsqrt(jnp.mean(stf * stf, axis=-1, keepdims=True) + EPS_NORM)
    nb[...] = (stf * inv).astype(BF)
    shift = lcol_ref[:, 0:1] - math.log2(k)
    dn_buf[...] = jnp.zeros_like(dn_buf)
    bufs = (la, lb)

    def back(logit, et, base):
        n = logit.shape[1]
        q = jnp.exp2(logit * c2 - shift)
        hit = lax.broadcasted_iota(jnp.int32, (2 * R, n), 1) == tg_ref[...] - base
        dl = jnp.where(hit, q - k, q).astype(BF)
        dn_buf[...] += mm(dl, et)

    def first():
        fetch(0).wait()
        la[...] = mm_t(nb[...], ebuf[0])

    def stage(i, w, r, carry):
        fetch(i).wait()

        @pl.when(i + DEPTH - 1 < n_full)
        def _():
            fetch(i + DEPTH - 1).start()

        bufs[w][...] = mm_t(nb[...], ebuf[lax.rem(i, DEPTH + 1)])
        back(bufs[r][...], ebuf[lax.rem(i + DEPTH, DEPTH + 1)], (i - 1) * TV)
        return carry

    def last(r, carry):
        back(bufs[r][...], ebuf[(n_full - 1) % (DEPTH + 1)], (n_full - 1) * TV)
        return carry

    staged(n_full, first, stage, last)(0)
    rem_copy.wait()
    back(mm_t(nb[...], erem[...]), erem[...], n_full * TV)

    stf = st_ref[...].astype(F32)
    inv = lax.rsqrt(jnp.mean(stf * stf, axis=-1, keepdims=True) + EPS_NORM)
    nf = stf * inv
    dn = dn_buf[...]
    ds = inv * (dn - nf * jnp.mean(dn * nf, axis=-1, keepdims=True))
    dout = ds[R:].astype(BF)
    dn_buf[...] = ds
    g_in = (stf[:R] + e1_ref[...].astype(F32)).astype(BF)
    dg_ref[...] = dout.astype(F32)

    def mtp(f, carry):
        w1 = wi_ref[:, rows(f, tile)]
        _, slope = gelu_both(mm(g_in, w1))
        dpre = (mm_t(dout, wo_ref[rows(f, tile), :]) * slope).astype(BF)
        dg_ref[...] += mm_t(dpre, w1)
        return carry

    lax.fori_loop(0, wi_ref.shape[1] // tile, mtp, 0)
    dh_ref[...] = (dn_buf[0:R, :] + dg_ref[...]).astype(BF)


def grad_phase(TV, tile, st, e1, tg, lcol, mtp_up, mtp_down, emb, after):
    R, D = e1.shape
    V = emb.shape[0]
    return pl.pallas_call(
        functools.partial(grad_kernel, TV, tile),
        out_shape=(jax.ShapeDtypeStruct((R, D), BF), jax.ShapeDtypeStruct((R, D), F32)),
        in_specs=[VMEM] * 6 + [ANY] * 2,
        out_specs=(VMEM,) * 2,
        scratch_shapes=[
            pltpu.VMEM((DEPTH + 1, TV, D), BF),
            pltpu.VMEM((V % TV, D), BF),
            pltpu.VMEM((2 * R, TV), F32),
            pltpu.VMEM((2 * R, TV), F32),
            pltpu.VMEM((2 * R, D), BF),
            pltpu.VMEM((2 * R, D), F32),
            pltpu.SemaphoreType.DMA((DEPTH + 1,)),
            pltpu.SemaphoreType.DMA,
        ],
        compiler_params=pltpu.CompilerParams(vmem_limit_bytes=VMEM_MAX),
        cost_estimate=cost(R * D * V, V * D),
        name='heads_grad',
    )(st, e1, tg, lcol, mtp_up, mtp_down, emb, after)


def bwd_kernel(S, C, tile, row0, pre, dh_ref, xs_ref, wi_ref, wit_ref, wot_ref, nall_ref, lse_ref, tgt_ref, emb_ref, after_ref,
               ds_ref, dpre_ref, hid_ref, dx_ref, q_ref,
               ob, pbuf, hbuf, ebuf, acc_buf, esem, qsem, own_sem, send_sem, recv_sem, psem, hsem, bsend, brecv):
    n_rows = xs_ref.shape[0]
    own = dh_ref.shape[0]
    F = wi_ref.shape[1]
    n_chunk, per = n_rows // C, own // C
    me = greet_all(S)
    last = S - 1
    prv = lax.rem(me + S - 1, S)
    half = S // 2

    tv, _ = ebuf.shape[1:]
    nb, _, tb = lse_ref.shape
    n_q = q_ref.shape[0] // tv
    short = emb_ref.shape[0] - row0 - (n_q - 1) * tv
    n_unit = n_q * nb

    def fetch(t, go):
        slot = lax.rem(t, 2)

        @pl.when(t < n_q - 1)
        def _():
            cp = pltpu.make_async_copy(emb_ref.at[pl.ds(pl.multiple_of(row0 + t * tv, tv), tv)], ebuf.at[slot], esem.at[slot])
            cp.start() if go else cp.wait()

        @pl.when(t == n_q - 1)
        def _():
            cp = pltpu.make_async_copy(emb_ref.at[pl.ds(row0 + (n_q - 1) * tv, short)], ebuf.at[slot, pl.ds(0, short)], esem.at[slot])
            cp.start() if go else cp.wait()

    def q_copy(t):
        slot = lax.rem(t, 2)
        return pltpu.make_async_copy(acc_buf.at[slot], q_ref.at[rows(t, tv)], qsem.at[slot])

    def unit(u, carry):
        t = u // nb
        j = lax.rem(u, nb)
        slot = lax.rem(t, 2)

        @pl.when(j == 0)
        def _():
            fetch(t, False)
            fetch(t + 1, True)

            @pl.when(t >= 2)
            def _():
                q_copy(t - 2).wait()

        part = head_block(ebuf[slot], row0 + t * tv, nall_ref[rows(j, tb), :], lse_ref[j], tgt_ref[j])

        @pl.when(j == 0)
        def _():
            acc_buf[slot] = part

        @pl.when(j > 0)
        def _():
            acc_buf[slot] += part

        @pl.when(j == nb - 1)
        def _():
            q_copy(t).start()

        return carry

    def units(lo, hi):
        lax.fori_loop(jnp.minimum(lo, n_unit), jnp.minimum(hi, n_unit), unit, 0)

    fetch(0, True)

    @pl.when(me < last)
    def _():
        for j in range(per):
            rcopy(dh_ref.at[rows(j, C)], ds_ref.at[rows(me * per + j, C)], own_sem.at[j], recv_sem.at[me * per + j], last).start()

    @pl.when(me == last)
    def _():
        ds_ref[last * own:, :] = dh_ref[...]

    def spread(c, stop):
        def to(i, d):
            cp = rcopy(dx_ref.at[rows(c, C)], dx_ref.at[rows(c, C)], bsend.at[i, c], brecv.at[c], d)
            cp.wait_send() if stop else cp.start()

        @pl.when(lax.rem(me, 2) == 0)
        def _():
            to(0, me + 1)

        @pl.when((lax.rem(me, 2) == 0) & (me < half))
        def _():
            to(1, me + 2)

        @pl.when((me == 0) | ((lax.rem(me, 2) == 0) & (me > half + 2)))
        def _():
            to(2, lax.rem(me + S - 2, S))

    def out_copies(c):
        slot = lax.rem(c, 2)
        return (pltpu.make_async_copy(pbuf.at[slot], dpre_ref.at[rows(c, C)], psem.at[slot]),
                pltpu.make_async_copy(hbuf.at[slot], hid_ref.at[rows(c, C)], hsem.at[slot]))

    ahead = (last - me) * pre
    units(0, ahead)

    def step(c, carry):
        slot = lax.rem(c, 2)

        @pl.when(c >= 2)
        def _():
            for cp in out_copies(c - 2):
                cp.wait()

        @pl.when((me < last) | (c < last * per))
        def _():
            rcopy(ds_ref.at[rows(c, C)], ds_ref.at[rows(c, C)], send_sem.at[c], recv_sem.at[c], prv).wait_recv()

        x = xs_ref[rows(c, C), :]
        dout = ds_ref[rows(c, C), :]
        acc = dout.astype(F32)
        for f in range(0, F, tile):
            w1 = wi_ref[:, f:f + tile]
            hid, slope = gelu_both(mm(x, w1))
            dpre = (mm(dout, wot_ref[:, f:f + tile]) * slope).astype(BF)
            hbuf[slot, :, f:f + tile] = hid.astype(BF)
            pbuf[slot, :, f:f + tile] = dpre
            acc += mm(dpre, wit_ref[f:f + tile, :])
        res = acc.astype(BF)

        @pl.when(me > 0)
        def _():
            ob[rows(c, C), :] = res
            rcopy(ob.at[rows(c, C)], ds_ref.at[rows(c, C)], send_sem.at[c], recv_sem.at[c], prv).start()

        @pl.when(me == 0)
        def _():
            dx_ref[rows(c, C), :] = res
            spread(c, False)

        for cp in out_copies(c):
            cp.start()
        units(ahead + c, ahead + c + 1)
        return carry

    lax.fori_loop(0, n_chunk, step, 0)

    for c in (n_chunk - 2, n_chunk - 1):
        for cp in out_copies(c):
            cp.wait()

    @pl.when(me < last)
    def _():
        for j in range(per):
            rcopy(dh_ref.at[rows(j, C)], ds_ref.at[rows(me * per + j, C)], own_sem.at[j], recv_sem.at[me * per + j], last).wait_send()

    done = jnp.minimum(ahead + n_chunk, n_unit)
    left = (n_unit - done + n_chunk - 1) // n_chunk

    def drain(c, carry):
        @pl.when(me > 0)
        def _():
            rcopy(ob.at[rows(c, C)], ds_ref.at[rows(c, C)], send_sem.at[c], recv_sem.at[c], prv).wait_send()
            rcopy(dx_ref.at[rows(c, C)], dx_ref.at[rows(c, C)], bsend.at[0, c], brecv.at[c], prv).wait_recv()
            spread(c, False)

        units(done + c * left, done + (c + 1) * left)
        return carry

    lax.fori_loop(0, n_chunk, drain, 0)
    for t in range(max(n_q - 2, 0), n_q):
        q_copy(t).wait()

    def settle(c, carry):
        spread(c, True)
        return carry

    lax.fori_loop(0, n_chunk, settle, 0)
    dx_ref[n_rows:, :] = jnp.zeros((WIN, dx_ref.shape[1]), BF)


def backward(S, C, tile, row0, tv, pre, dh, xs, w_in, w_in_t, w_out_t, nall, lse, tgt, emb, after):
    own, D = dh.shape
    n_rows = xs.shape[0]
    F = w_in.shape[1]
    n_chunk, per = n_rows // C, own // C
    n_q = pl.cdiv(emb.shape[0] - row0, tv)
    return pl.pallas_call(
        functools.partial(bwd_kernel, S, C, tile, row0, pre),
        out_shape=(jax.ShapeDtypeStruct((n_rows, D), BF), jax.ShapeDtypeStruct((n_rows, F), BF),
                   jax.ShapeDtypeStruct((n_rows, F), BF), jax.ShapeDtypeStruct((n_rows + WIN, D), BF),
                   jax.ShapeDtypeStruct((n_q * tv, D), F32)),
        in_specs=[VMEM] * 8 + [ANY] * 2,
        out_specs=(VMEM, ANY, ANY, VMEM, ANY),
        scratch_shapes=[
            pltpu.VMEM((n_rows, D), BF),
            pltpu.VMEM((2, C, F), BF),
            pltpu.VMEM((2, C, F), BF),
            pltpu.VMEM((2, tv, D), BF),
            pltpu.VMEM((2, tv, D), F32),
            pltpu.SemaphoreType.DMA((2,)),
            pltpu.SemaphoreType.DMA((2,)),
            pltpu.SemaphoreType.DMA((per,)),
            pltpu.SemaphoreType.DMA((n_chunk,)),
            pltpu.SemaphoreType.DMA((n_chunk,)),
            pltpu.SemaphoreType.DMA((2,)),
            pltpu.SemaphoreType.DMA((2,)),
            pltpu.SemaphoreType.DMA((3, n_chunk)),
            pltpu.SemaphoreType.DMA((n_chunk,)),
        ],
        compiler_params=pltpu.CompilerParams(collective_id=2, has_side_effects=True, vmem_limit_bytes=VMEM_MAX),
        cost_estimate=cost(n_rows * w_in.size, n_rows * F),
        name='bwd_pipe',
    )(dh, xs, w_in, w_in_t, w_out_t, nall, lse, tgt, emb, after)


def head_block(et, base, rows_j, lse_j, tgt_j):
    D = et.shape[1]
    k = 0.5 * D ** -0.5
    q = jnp.exp2(mm_t(et, rows_j) * (D ** -0.5 * math.log2(math.e)) - (lse_j - math.log2(k)))
    hit = lax.broadcasted_iota(jnp.int32, q.shape, 0) == tgt_j - base
    return mm(jnp.where(hit, q - k, q).astype(BF), rows_j)


def shard_kernel(off_ref, e_ref, nall_ref, lse_ref, tgt_ref, after_ref, o_ref):
    tv = e_ref.shape[0]
    nb, _, tb = lse_ref.shape
    base = (off_ref[0] + pl.program_id(0)) * tv
    o_ref[...] = head_block(e_ref[...], base, nall_ref[0:tb, :], lse_ref[0], tgt_ref[0])

    def body(j, carry):
        o_ref[...] += head_block(e_ref[...], base, nall_ref[rows(j, tb), :], lse_ref[j], tgt_ref[j])
        return carry

    lax.fori_loop(1, nb, body, 0)


def head_shard(tv, n_tile, off, emb, nall, lse, tgt, after):
    D = emb.shape[1]
    return pl.pallas_call(
        shard_kernel,
        out_shape=jax.ShapeDtypeStruct((n_tile * tv, D), F32),
        grid_spec=pltpu.PrefetchScalarGridSpec(
            num_scalar_prefetch=1, grid=(n_tile,),
            in_specs=[pl.BlockSpec((tv, D), lambda i, o: (o[0] + i, 0)), VMEM, VMEM, VMEM, ANY],
            out_specs=pl.BlockSpec((tv, D), lambda i, o: (i, 0))),
        compiler_params=pltpu.CompilerParams(vmem_limit_bytes=VMEM_MAX),
        cost_estimate=cost(n_tile * tv * nall.size, n_tile * tv * D),
        name='head_shard',
    )(off, emb, nall, lse, tgt, after)


def split3(v):
    hi = v.astype(BF)
    rest = v - hi.astype(F32)
    mid = rest.astype(BF)
    return [hi, mid, (rest - mid.astype(F32)).astype(BF)]


def place(t, parts):
    at, base = t, 0
    for first, n in parts:
        at = jnp.where(t >= base, first + t - base, at)
        base += n
    return at


def sweep_kernel(tv, parts, lim_ref, tokw_ref, dx_ref, labw_ref, dg_ref, *refs):
    a_refs, o_ref = refs[:len(parts)], refs[-1]
    t = pl.program_id(0)
    tile0 = place(t, parts) * SUB
    top = tokw_ref.shape[0] - 1

    def part(s, i):
        tile = jnp.minimum(tile0 + s, lim_ref.shape[1] - 1)
        wt = jnp.minimum(lim_ref[0, tile] + i * (WIN // STEP), top)
        wl = jnp.minimum(lim_ref[1, tile] + i * (WIN // STEP), top)
        ids = jnp.maximum(tokw_ref[pl.ds(wt, 1), :], labw_ref[pl.ds(wl, 1), :]) - (tile0 + s) * tv
        hit = lax.broadcasted_iota(jnp.int32, (tv, 4 * WIN), 0) == ids
        near = pl.ds(pl.multiple_of(wt * STEP, STEP), WIN)
        far = pl.ds(pl.multiple_of(wl * STEP, STEP), WIN)
        return mm(jnp.where(hit, 1.0, 0.0).astype(BF), jnp.concatenate([dx_ref[near, :]] + split3(dg_ref[far, :]), axis=0))

    base = 0
    for (first, n), a_ref in zip(parts, a_refs):
        @pl.when((t >= base) & (t < base + n))
        def _():
            for s in range(SUB):
                o_ref[s * tv:(s + 1) * tv, :] = a_ref[s * tv:(s + 1) * tv, :] + part(s, 0)

        base += n

    for s in range(SUB):
        def more(i, carry):
            o_ref[s * tv:(s + 1) * tv, :] += part(s, i)
            return carry

        lax.fori_loop(1, lim_ref[2, jnp.minimum(tile0 + s, lim_ref.shape[1] - 1)], more, 0)


def sweep(tv, parts, arrays, lim, tokw, dx, labw, dg, out_rows, full):
    D = dx.shape[1]
    size = SUB * tv
    keep = [] if full is None else [full]
    specs, base = [], 0
    for first, n in parts:
        specs.append(pl.BlockSpec((size, D), lambda t, base=base, n=n: (jnp.clip(t - base, 0, n - 1), 0)))
        base += n
    return pl.pallas_call(
        functools.partial(sweep_kernel, tv, parts),
        out_shape=jax.ShapeDtypeStruct((out_rows, D), F32),
        grid=(base,),
        in_specs=[SMEM] + [VMEM] * 4 + specs + [ANY] * len(keep),
        out_specs=pl.BlockSpec((size, D), lambda t: (place(t, parts), 0)),
        input_output_aliases={5 + len(parts): 0} if keep else {},
        compiler_params=pltpu.CompilerParams(vmem_limit_bytes=VMEM_MAX),
        cost_estimate=cost(base * size * D, base * size * D),
        name='sweep',
    )(lim, tokw, dx, labw, dg, *arrays, *keep)


def windows(sorted_ids, slots):
    pad = jnp.pad(sorted_ids, (0, WIN), constant_values=-1).reshape(-1, STEP)
    n = sorted_ids.size // STEP
    win = jnp.concatenate([pad[i:i + n] for i in range(WIN // STEP)], axis=1)
    none = jnp.full_like(win, -1)
    return jnp.pad(jnp.concatenate([win if s else none for s in slots], axis=1), ((0, 1), (0, 0)), constant_values=-1)


def limits(tok, lab, tv, n_tile):
    edge = jnp.arange(n_tile + 1, dtype=jnp.int32) * tv

    def span(ids):
        below = jnp.sum((ids[None, :] < edge[:, None]).astype(jnp.int32), axis=1)
        w = below[:-1] // STEP
        return w, (below[1:] - w * STEP + WIN - 1) // WIN

    wt, nt = span(tok)
    wl, nl = span(lab)
    return jnp.stack([wt, wl, jnp.maximum(nt, nl)])


TILE_V = 512
TOKENS = 1024
WIN = 64
STEP = 16
AHEAD = 4
SUB = 2
PIECES = (2, 3, 1)
FWD_ROWS = 128
BWD_ROWS = 128


def solution(mesh):
    S = mesh.shape[AXIS]

    def per_device(token_ids, label_ids, label2_ids, embed_table, w_up, w_down, mtp_up, mtp_down):
        V, D = embed_table.shape
        N = token_ids.size
        R = N // S
        me = lax.axis_index(AXIS)
        w_in, w_out = w_up[0], w_down[0]

        tok, lab, lab2 = lax.sort((token_ids.reshape(N), label_ids.reshape(N), label2_ids.reshape(N)), num_keys=1)

        def own(v):
            return lax.dynamic_slice_in_dim(v, me * R, R)

        picked = embed_table[jnp.concatenate([own(tok), own(lab), own(lab2)])]
        x_own, e1, e2 = picked[:R], picked[R:2 * R], picked[2 * R:]
        xs, h_own, w_in_t, w_out_t = forward(S, FWD_ROWS, 1024, x_own, w_in, w_out)
        tg = jnp.concatenate([own(lab), own(lab2)]).reshape(2 * R, 1)
        nall, lall, st, lcol = lse_phase(S, 1024, 1024, h_own, e1, e2, mtp_up, mtp_down, embed_table)
        nall = nall.reshape(2 * N, D)
        lse = lall[:, 0, :].reshape(2 * N // TOKENS, 1, TOKENS)
        tgt = jnp.stack([lab.reshape(S, R), lab2.reshape(S, R)], axis=1).reshape(2 * N // TOKENS, 1, TOKENS)

        starts = [S * sum(PIECES[:i]) for i in range(len(PIECES) + 1)]

        def piece(i, after):
            off = (starts[i] + me * PIECES[i]).reshape(1)
            return head_shard(TILE_V, PIECES[i], off, embed_table, nall, lse, tgt, after)

        def share(v):
            return lax.all_gather(v, AXIS, axis=0, tiled=True)

        mine = [piece(0, lcol)]
        gathered = [share(mine[0])]
        dh, dg = grad_phase(1024, 1024, st, e1, tg, lcol, mtp_up, mtp_down, embed_table, mine[0])
        for i in range(1, len(PIECES)):
            mine.append(piece(i, dg if i == 1 else mine[-1]))
            gathered.append(share(mine[-1]))
            if i == 1:
                dg_all = share(dg)

        dsv, dpre, hid, dx, q_part = backward(S, BWD_ROWS, 1024, starts[-1] * TILE_V, TILE_V, AHEAD, dh, xs, w_in, w_in_t, w_out_t, nall, lse, tgt, embed_table, mine[-1])
        g_up = lax.dot_general(xs, dpre, (((0,), (0,)), ((), ())), preferred_element_type=F32)
        g_down = lax.dot_general(hid, dsv, (((0,), (0,)), ((), ())), preferred_element_type=F32)
        loss = (0.5 * jnp.sum(lall[:, 1, 0]) / N).reshape(1)

        lab_sorted, lab_perm = lax.sort((lab, lax.iota(jnp.int32, N)), num_keys=1)
        dg_rows = dg_all[jnp.pad(lab_perm, (0, WIN))]
        n_tile = pl.cdiv(V, TILE_V)
        lim = limits(tok, lab_sorted, TILE_V, n_tile)
        tokw = windows(tok, (1, 0, 0, 0))
        labw = windows(lab_sorted, (0, 1, 1, 1))
        ends = starts[1:] + [pl.cdiv(n_tile, SUB) * SUB]
        span = [(a // SUB, (b - a) // SUB) for a, b in zip(starts, ends)]
        early = [0, 1, len(PIECES)]
        stock = gathered + [q_part]
        full = sweep(TILE_V, [span[i] for i in early], [stock[i] for i in early], lim, tokw, dx, labw, dg_rows, V, None)
        for i in range(2, len(PIECES)):
            full = sweep(TILE_V, [span[i]], [stock[i]], lim, tokw, dx, labw, dg_rows, V, full)
        return loss, g_up[None], g_down[None], full

    in_specs = (P('dp'),) * 3 + (P(), P('stage'), P('stage'), P(), P())
    out_specs = (P('dp'), P(('dp', 'stage')), P(('dp', 'stage')), P('dp'))
    return jax.shard_map(per_device, mesh=mesh, in_specs=in_specs, out_specs=out_specs, check_vma=False)
```

```python
import functools
import math

import jax
import jax.numpy as jnp
from jax import lax
from jax.experimental import pallas as pl
from jax.experimental.pallas import tpu as pltpu
from jax.sharding import PartitionSpec as P


EPS_NORM = 1e-6
BF = jnp.bfloat16
F32 = jnp.float32
AXIS = 'stage'
GELU_A = math.sqrt(2.0 / math.pi)
GELU_B = 0.044715
VMEM_MAX = 67000000
DEPTH = 4

VMEM = pl.BlockSpec(memory_space=pltpu.VMEM)
ANY = pl.BlockSpec(memory_space=pl.ANY)
SMEM = pl.BlockSpec(memory_space=pltpu.SMEM)
NN = (((1,), (0,)), ((), ()))
NT = (((1,), (1,)), ((), ()))


def cost(work, elems):
    return pl.CostEstimate(flops=8 * work, bytes_accessed=8 * elems, transcendentals=0)


def mm(a, b):
    return lax.dot_general(a, b, NN, preferred_element_type=F32)


def mm_t(a, b):
    return lax.dot_general(a, b, NT, preferred_element_type=F32)


def gelu(v):
    return 0.5 * v * (1.0 + jnp.tanh(GELU_A * (v + GELU_B * (v * v * v))))


def gelu_both(v):
    sq = v * v
    t = jnp.tanh(GELU_A * (v + GELU_B * (sq * v)))
    half = 0.5 * (1.0 + t)
    slope = half + (0.5 * v) * (1.0 - t * t) * (GELU_A * (1.0 + (3.0 * GELU_B) * sq))
    return v * half, slope


def dev(d):
    return {AXIS: d}


def greet_all(n_dev):
    me = lax.axis_index(AXIS)
    bar = pltpu.get_barrier_semaphore()
    for d in range(1, n_dev):
        pl.semaphore_signal(bar, inc=1, device_id=dev(lax.rem(me + d, n_dev)), device_id_type=pl.DeviceIdType.MESH)
    pl.semaphore_wait(bar, n_dev - 1)
    return me


def rcopy(src, dst, ssem, rsem, d):
    return pltpu.make_async_remote_copy(src_ref=src, dst_ref=dst, send_sem=ssem, recv_sem=rsem, device_id=dev(d), device_id_type=pl.DeviceIdType.MESH)


def rows(c, size):
    return pl.ds(pl.multiple_of(c * size, size), size)


def mlp_rows(x, wi_ref, wo_ref, tile):
    acc = None
    for f in range(0, wi_ref.shape[1], tile):
        hid = gelu(mm(x, wi_ref[:, f:f + tile])).astype(BF)
        part = mm(hid, wo_ref[f:f + tile, :])
        acc = part if acc is None else acc + part
    return (x.astype(F32) + acc).astype(BF)


def fwd_kernel(S, C, tile, x_ref, wi_ref, wo_ref, xs_ref, h_ref, wit_ref, wot_ref, ob, own_sem, send_sem, recv_sem, h_sem):
    n_rows = xs_ref.shape[0]
    own = x_ref.shape[0]
    n_chunk, per = n_rows // C, own // C
    me = greet_all(S)
    nxt = lax.rem(me + 1, S)

    def flip(f, carry):
        wit_ref[rows(f, 512), :] = jnp.transpose(wi_ref[:, rows(f, 512)])
        wot_ref[:, rows(f, 512)] = jnp.transpose(wo_ref[rows(f, 512), :])
        return carry

    early = me >= S // 2

    @pl.when(me > 0)
    def _():
        for j in range(per):
            rcopy(x_ref.at[rows(j, C)], xs_ref.at[rows(me * per + j, C)], own_sem.at[j], recv_sem.at[me * per + j], 0).start()

    @pl.when(me == 0)
    def _():
        xs_ref[0:own, :] = x_ref[...]

    lax.fori_loop(0, jnp.where(early, wi_ref.shape[1] // 512, 0), flip, 0)

    def step(c, carry):
        @pl.when((me > 0) | (c >= per))
        def _():
            rcopy(xs_ref.at[rows(c, C)], xs_ref.at[rows(c, C)], send_sem.at[c], recv_sem.at[c], nxt).wait_recv()

        ob[rows(c, C), :] = mlp_rows(xs_ref[rows(c, C), :], wi_ref, wo_ref, tile)
        owner = c // per
        j = lax.rem(c, per)

        @pl.when(me < S - 1)
        def _():
            rcopy(ob.at[rows(c, C)], xs_ref.at[rows(c, C)], send_sem.at[c], recv_sem.at[c], nxt).start()

        @pl.when((me == S - 1) & (owner < S - 1))
        def _():
            rcopy(ob.at[rows(c, C)], h_ref.at[rows(j, C)], send_sem.at[c], h_sem.at[j], owner).start()

        @pl.when((me == S - 1) & (owner == S - 1))
        def _():
            h_ref[rows(j, C), :] = ob[rows(c, C), :]

        return carry

    lax.fori_loop(0, n_chunk, step, 0)

    @pl.when(me > 0)
    def _():
        for j in range(per):
            rcopy(x_ref.at[rows(j, C)], xs_ref.at[rows(me * per + j, C)], own_sem.at[j], recv_sem.at[me * per + j], 0).wait_send()

    def drain(c, carry):
        @pl.when((me < S - 1) | (c < (S - 1) * per))
        def _():
            rcopy(ob.at[rows(c, C)], xs_ref.at[rows(c, C)], send_sem.at[c], recv_sem.at[c], nxt).wait_send()

        return carry

    lax.fori_loop(0, jnp.where(early, 0, wi_ref.shape[1] // 512), flip, 0)
    lax.fori_loop(0, n_chunk, drain, 0)

    @pl.when(me < S - 1)
    def _():
        for j in range(per):
            rcopy(ob.at[rows(j, C)], h_ref.at[rows(j, C)], send_sem.at[j], h_sem.at[j], nxt).wait_recv()


def forward(S, C, tile, x_own, w_in, w_out):
    own, width = x_own.shape
    n_rows = own * S
    n_chunk, per = n_rows // C, own // C
    return pl.pallas_call(
        functools.partial(fwd_kernel, S, C, tile),
        out_shape=(jax.ShapeDtypeStruct((n_rows, width), BF), jax.ShapeDtypeStruct((own, width), BF),
                   jax.ShapeDtypeStruct(w_out.shape, BF), jax.ShapeDtypeStruct(w_in.shape, BF)),
        in_specs=[VMEM] * 3,
        out_specs=(VMEM,) * 4,
        scratch_shapes=[
            pltpu.VMEM((n_rows, width), BF),
            pltpu.SemaphoreType.DMA((per,)),
            pltpu.SemaphoreType.DMA((n_chunk,)),
            pltpu.SemaphoreType.DMA((n_chunk,)),
            pltpu.SemaphoreType.DMA((per,)),
        ],
        compiler_params=pltpu.CompilerParams(collective_id=0, has_side_effects=True, vmem_limit_bytes=VMEM_MAX),
        cost_estimate=cost(n_rows * w_in.size, w_in.size),
        name='fwd_pipe',
    )(x_own, w_in, w_out)


def stream(emb_ref, ebuf, esem, TV):
    def fetch(i):
        slot = lax.rem(i, ebuf.shape[0])
        return pltpu.make_async_copy(emb_ref.at[rows(i, TV)], ebuf.at[slot], esem.at[slot])

    return fetch


def staged(n_full, first, stage, last):
    first()

    def pair(j, carry):
        carry = stage(2 * j + 1, 1, 0, carry)
        return stage(2 * j + 2, 0, 1, carry)

    return lambda carry: tail(n_full, stage, last, lax.fori_loop(0, (n_full - 1) // 2, pair, carry))


def tail(n_full, stage, last, carry):
    if (n_full - 1) % 2:
        carry = stage(n_full - 1, 1, 0, carry)
    return last((n_full - 1) % 2, carry)


def lse_kernel(S, TV, tile, h_ref, e1_ref, e2_ref, wi_ref, wo_ref, emb_ref,
               nall_ref, lall_ref, st_ref, lcol_ref,
               ebuf, erem, la, lb, lrow, esem, rsem, nsend, nrecv, lsend, lrecv):
    R, D = h_ref.shape
    V = emb_ref.shape[0]
    n_full = V // TV
    rem = V - n_full * TV
    scale = D ** -0.5
    c2 = scale * math.log2(math.e)
    me = greet_all(S)
    fetch = stream(emb_ref, ebuf, esem, TV)
    for i in range(DEPTH):
        fetch(i).start()
    rem_copy = pltpu.make_async_copy(emb_ref.at[pl.ds(n_full * TV, rem)], erem, rsem)
    rem_copy.start()

    hf = h_ref[...].astype(F32)
    st_ref[0:R, :] = h_ref[...]
    g_in = (hf + e1_ref[...].astype(F32)).astype(BF)
    acc_ref = la.at[pl.ds(0, R)]
    acc_ref[...] = jnp.zeros((R, D), F32)

    def mtp(f, carry):
        acc_ref[...] += mm(gelu(mm(g_in, wi_ref[:, rows(f, tile)])).astype(BF), wo_ref[rows(f, tile), :])
        return carry

    lax.fori_loop(0, wi_ref.shape[1] // tile, mtp, 0)
    g_out = (g_in.astype(F32) + acc_ref[...]).astype(BF)
    st_ref[R:, :] = g_out
    for j, v in enumerate((hf, g_out.astype(F32))):
        inv = lax.rsqrt(jnp.mean(v * v, axis=-1, keepdims=True) + EPS_NORM)
        nall_ref[me, j * R:(j + 1) * R, :] = (v * inv).astype(BF)

    sib = me + 1 - 2 * lax.rem(me, 2)

    def block(b, ssem, d):
        return rcopy(nall_ref.at[b], nall_ref.at[b], ssem, nrecv.at[b], d)

    def peer(d):
        return lax.rem(me + 2 * d, S)

    def lcopy(d):
        return rcopy(lall_ref.at[me], lall_ref.at[me], lsend.at[d], lrecv.at[d], lax.rem(me + d, S))

    for d in range(1, S // 2):
        block(me, nsend.at[d], peer(d)).start()
    block(me, nsend.at[0], sib).start()

    bufs = (la, lb)

    def fold(lt, mx, sm):
        grp = lt.reshape(lt.shape[0] // 8, 8, 2 * R)
        new = jnp.maximum(mx, jnp.max(grp, axis=0))
        sm = sm * jnp.exp2((mx - new) * c2) + jnp.sum(jnp.exp2((grp - new[None]) * c2), axis=0)
        return new, sm

    def first():
        fetch(0).wait()
        la[...] = mm_t(ebuf[0], nall_ref[me])

    def stage(i, w, r, carry):
        fetch(i).wait()

        @pl.when(i + DEPTH - 1 < n_full)
        def _():
            fetch(i + DEPTH - 1).start()

        bufs[w][...] = mm_t(ebuf[lax.rem(i, ebuf.shape[0])], nall_ref[me])
        return fold(bufs[r][...], *carry)

    def last(r, carry):
        return fold(bufs[r][...], *carry)

    mx, sm = staged(n_full, first, stage, last)((jnp.full((8, 2 * R), -jnp.inf, F32), jnp.zeros((8, 2 * R), F32)))
    for d in range(1, S // 2):
        block(peer(d), nsend.at[S // 2 + d], sib).wait_recv()
        block(peer(d), nsend.at[S // 2 + d], sib).start()
    rem_copy.wait()
    mx, sm = fold(mm_t(erem[...], nall_ref[me]), mx, sm)
    top = jnp.max(mx, axis=0, keepdims=True)
    tot = jnp.sum(sm * jnp.exp2((mx - top) * c2), axis=0, keepdims=True)
    lse2 = top * c2 + jnp.log(tot) * math.log2(math.e)
    lrow[...] = jnp.broadcast_to(lse2, (128, 2 * R))
    lcol_ref[...] = jnp.transpose(lrow[...])
    nrm = nall_ref[me].astype(F32)
    pick = jnp.concatenate([
        jnp.sum(nrm[:R] * e1_ref[...].astype(F32), axis=-1, keepdims=True),
        jnp.sum(nrm[R:] * e2_ref[...].astype(F32), axis=-1, keepdims=True)], axis=0) * scale
    nll = jnp.sum(lcol_ref[:, 0:1] * math.log(2.0) - pick, axis=0, keepdims=True)
    lall_ref[me] = jnp.where(lax.broadcasted_iota(jnp.int32, (8, 2 * R), 0) == 0, jnp.broadcast_to(lse2, (8, 2 * R)), jnp.broadcast_to(nll, (8, 2 * R)))
    for d in range(1, S):
        lcopy(d).start()
    for d in range(1, S // 2):
        block(me, nsend.at[d], peer(d)).wait_send()
        block(peer(d), nsend.at[S // 2 + d], sib).wait_send()
        block(lax.rem(sib + 2 * d, S), nsend.at[d], sib).wait_recv()
    block(me, nsend.at[0], sib).wait_send()
    block(sib, nsend.at[0], sib).wait_recv()
    for d in range(1, S):
        lcopy(d).wait_send()
        src = lax.rem(me + S - d, S)
        rcopy(lall_ref.at[me], lall_ref.at[src], lsend.at[d], lrecv.at[d], lax.rem(me + d, S)).wait_recv()


def lse_phase(S, TV, tile, h_own, e1, e2, mtp_up, mtp_down, emb):
    R, D = h_own.shape
    V = emb.shape[0]
    return pl.pallas_call(
        functools.partial(lse_kernel, S, TV, tile),
        out_shape=(jax.ShapeDtypeStruct((S, 2 * R, D), BF), jax.ShapeDtypeStruct((S, 8, 2 * R), F32),
                   jax.ShapeDtypeStruct((2 * R, D), BF), jax.ShapeDtypeStruct((2 * R, 128), F32)),
        in_specs=[VMEM] * 5 + [ANY],
        out_specs=(VMEM,) * 4,
        scratch_shapes=[
            pltpu.VMEM((DEPTH, TV, D), BF),
            pltpu.VMEM((V % TV, D), BF),
            pltpu.VMEM((TV, 2 * R), F32),
            pltpu.VMEM((TV, 2 * R), F32),
            pltpu.VMEM((128, 2 * R), F32),
            pltpu.SemaphoreType.DMA((DEPTH,)),
            pltpu.SemaphoreType.DMA,
            pltpu.SemaphoreType.DMA((S,)),
            pltpu.SemaphoreType.DMA((S,)),
            pltpu.SemaphoreType.DMA((S,)),
            pltpu.SemaphoreType.DMA((S,)),
        ],
        compiler_params=pltpu.CompilerParams(collective_id=1, has_side_effects=True, vmem_limit_bytes=VMEM_MAX),
        cost_estimate=cost(R * D * V, V * D),
        name='heads_lse',
    )(h_own, e1, e2, mtp_up, mtp_down, emb)


def grad_kernel(TV, tile, st_ref, e1_ref, tg_ref, lcol_ref, wi_ref, wo_ref, emb_ref, after_ref,
                dh_ref, dg_ref, ebuf, erem, la, lb, nb, dn_buf, esem, rsem):
    R, D = e1_ref.shape
    V = emb_ref.shape[0]
    n_full = V // TV
    rem = V - n_full * TV
    scale = D ** -0.5
    c2 = scale * math.log2(math.e)
    k = 0.5 * scale
    fetch = stream(emb_ref, ebuf, esem, TV)
    for i in range(DEPTH):
        fetch(i).start()
    rem_copy = pltpu.make_async_copy(emb_ref.at[pl.ds(n_full * TV, rem)], erem, rsem)
    rem_copy.start()
    stf = st_ref[...].astype(F32)
    inv = lax.rsqrt(jnp.mean(stf * stf, axis=-1, keepdims=True) + EPS_NORM)
    nb[...] = (stf * inv).astype(BF)
    shift = lcol_ref[:, 0:1] - math.log2(k)
    dn_buf[...] = jnp.zeros_like(dn_buf)
    bufs = (la, lb)

    def back(logit, et, base):
        n = logit.shape[1]
        q = jnp.exp2(logit * c2 - shift)
        hit = lax.broadcasted_iota(jnp.int32, (2 * R, n), 1) == tg_ref[...] - base
        dl = jnp.where(hit, q - k, q).astype(BF)
        dn_buf[...] += mm(dl, et)

    def first():
        fetch(0).wait()
        la[...] = mm_t(nb[...], ebuf[0])

    def stage(i, w, r, carry):
        fetch(i).wait()

        @pl.when(i + DEPTH - 1 < n_full)
        def _():
            fetch(i + DEPTH - 1).start()

        bufs[w][...] = mm_t(nb[...], ebuf[lax.rem(i, DEPTH + 1)])
        back(bufs[r][...], ebuf[lax.rem(i + DEPTH, DEPTH + 1)], (i - 1) * TV)
        return carry

    def last(r, carry):
        back(bufs[r][...], ebuf[(n_full - 1) % (DEPTH + 1)], (n_full - 1) * TV)
        return carry

    staged(n_full, first, stage, last)(0)
    rem_copy.wait()
    back(mm_t(nb[...], erem[...]), erem[...], n_full * TV)

    stf = st_ref[...].astype(F32)
    inv = lax.rsqrt(jnp.mean(stf * stf, axis=-1, keepdims=True) + EPS_NORM)
    nf = stf * inv
    dn = dn_buf[...]
    ds = inv * (dn - nf * jnp.mean(dn * nf, axis=-1, keepdims=True))
    dout = ds[R:].astype(BF)
    dn_buf[...] = ds
    g_in = (stf[:R] + e1_ref[...].astype(F32)).astype(BF)
    dg_ref[...] = dout.astype(F32)

    def mtp(f, carry):
        w1 = wi_ref[:, rows(f, tile)]
        _, slope = gelu_both(mm(g_in, w1))
        dpre = (mm_t(dout, wo_ref[rows(f, tile), :]) * slope).astype(BF)
        dg_ref[...] += mm_t(dpre, w1)
        return carry

    lax.fori_loop(0, wi_ref.shape[1] // tile, mtp, 0)
    dh_ref[...] = (dn_buf[0:R, :] + dg_ref[...]).astype(BF)


def grad_phase(TV, tile, st, e1, tg, lcol, mtp_up, mtp_down, emb, after):
    R, D = e1.shape
    V = emb.shape[0]
    return pl.pallas_call(
        functools.partial(grad_kernel, TV, tile),
        out_shape=(jax.ShapeDtypeStruct((R, D), BF), jax.ShapeDtypeStruct((R, D), F32)),
        in_specs=[VMEM] * 6 + [ANY] * 2,
        out_specs=(VMEM,) * 2,
        scratch_shapes=[
            pltpu.VMEM((DEPTH + 1, TV, D), BF),
            pltpu.VMEM((V % TV, D), BF),
            pltpu.VMEM((2 * R, TV), F32),
            pltpu.VMEM((2 * R, TV), F32),
            pltpu.VMEM((2 * R, D), BF),
            pltpu.VMEM((2 * R, D), F32),
            pltpu.SemaphoreType.DMA((DEPTH + 1,)),
            pltpu.SemaphoreType.DMA,
        ],
        compiler_params=pltpu.CompilerParams(vmem_limit_bytes=VMEM_MAX),
        cost_estimate=cost(R * D * V, V * D),
        name='heads_grad',
    )(st, e1, tg, lcol, mtp_up, mtp_down, emb, after)


def bwd_kernel(S, C, tile, row0, pre, dh_ref, xs_ref, wi_ref, wit_ref, wot_ref, nall_ref, lse_ref, tgt_ref, emb_ref, after_ref,
               ds_ref, dpre_ref, hid_ref, dx_ref, q_ref,
               ob, pbuf, hbuf, ebuf, acc_buf, esem, qsem, own_sem, send_sem, recv_sem, psem, hsem, bsend, brecv):
    n_rows = xs_ref.shape[0]
    own = dh_ref.shape[0]
    F = wi_ref.shape[1]
    n_chunk, per = n_rows // C, own // C
    me = greet_all(S)
    last = S - 1
    prv = lax.rem(me + S - 1, S)
    half = S // 2

    tv, _ = ebuf.shape[1:]
    nb, _, tb = lse_ref.shape
    n_q = q_ref.shape[0] // tv
    short = emb_ref.shape[0] - row0 - (n_q - 1) * tv
    n_unit = n_q * nb

    def fetch(t, go):
        slot = lax.rem(t, 2)

        @pl.when(t < n_q - 1)
        def _():
            cp = pltpu.make_async_copy(emb_ref.at[pl.ds(pl.multiple_of(row0 + t * tv, tv), tv)], ebuf.at[slot], esem.at[slot])
            cp.start() if go else cp.wait()

        @pl.when(t == n_q - 1)
        def _():
            cp = pltpu.make_async_copy(emb_ref.at[pl.ds(row0 + (n_q - 1) * tv, short)], ebuf.at[slot, pl.ds(0, short)], esem.at[slot])
            cp.start() if go else cp.wait()

    def q_copy(t):
        slot = lax.rem(t, 2)
        return pltpu.make_async_copy(acc_buf.at[slot], q_ref.at[rows(t, tv)], qsem.at[slot])

    def unit(u, carry):
        t = u // nb
        j = lax.rem(u, nb)
        slot = lax.rem(t, 2)

        @pl.when(j == 0)
        def _():
            fetch(t, False)
            fetch(t + 1, True)

            @pl.when(t >= 2)
            def _():
                q_copy(t - 2).wait()

        part = head_block(ebuf[slot], row0 + t * tv, nall_ref[rows(j, tb), :], lse_ref[j], tgt_ref[j])

        @pl.when(j == 0)
        def _():
            acc_buf[slot] = part

        @pl.when(j > 0)
        def _():
            acc_buf[slot] += part

        @pl.when(j == nb - 1)
        def _():
            q_copy(t).start()

        return carry

    def units(lo, hi):
        lax.fori_loop(jnp.minimum(lo, n_unit), jnp.minimum(hi, n_unit), unit, 0)

    fetch(0, True)

    @pl.when(me < last)
    def _():
        for j in range(per):
            rcopy(dh_ref.at[rows(j, C)], ds_ref.at[rows(me * per + j, C)], own_sem.at[j], recv_sem.at[me * per + j], last).start()

    @pl.when(me == last)
    def _():
        ds_ref[last * own:, :] = dh_ref[...]

    def spread(c, stop):
        def to(i, d):
            cp = rcopy(dx_ref.at[rows(c, C)], dx_ref.at[rows(c, C)], bsend.at[i, c], brecv.at[c], d)
            cp.wait_send() if stop else cp.start()

        @pl.when(lax.rem(me, 2) == 0)
        def _():
            to(0, me + 1)

        @pl.when((lax.rem(me, 2) == 0) & (me < half))
        def _():
            to(1, me + 2)

        @pl.when((me == 0) | ((lax.rem(me, 2) == 0) & (me > half + 2)))
        def _():
            to(2, lax.rem(me + S - 2, S))

    def out_copies(c):
        slot = lax.rem(c, 2)
        return (pltpu.make_async_copy(pbuf.at[slot], dpre_ref.at[rows(c, C)], psem.at[slot]),
                pltpu.make_async_copy(hbuf.at[slot], hid_ref.at[rows(c, C)], hsem.at[slot]))

    ahead = (last - me) * pre
    units(0, ahead)

    def step(c, carry):
        slot = lax.rem(c, 2)

        @pl.when(c >= 2)
        def _():
            for cp in out_copies(c - 2):
                cp.wait()

        @pl.when((me < last) | (c < last * per))
        def _():
            rcopy(ds_ref.at[rows(c, C)], ds_ref.at[rows(c, C)], send_sem.at[c], recv_sem.at[c], prv).wait_recv()

        x = xs_ref[rows(c, C), :]
        dout = ds_ref[rows(c, C), :]
        acc = dout.astype(F32)
        for f in range(0, F, tile):
            w1 = wi_ref[:, f:f + tile]
            hid, slope = gelu_both(mm(x, w1))
            dpre = (mm(dout, wot_ref[:, f:f + tile]) * slope).astype(BF)
            hbuf[slot, :, f:f + tile] = hid.astype(BF)
            pbuf[slot, :, f:f + tile] = dpre
            acc += mm(dpre, wit_ref[f:f + tile, :])
        res = acc.astype(BF)

        @pl.when(me > 0)
        def _():
            ob[rows(c, C), :] = res
            rcopy(ob.at[rows(c, C)], ds_ref.at[rows(c, C)], send_sem.at[c], recv_sem.at[c], prv).start()

        @pl.when(me == 0)
        def _():
            dx_ref[rows(c, C), :] = res
            spread(c, False)

        for cp in out_copies(c):
            cp.start()
        units(ahead + c * PER_CHUNK, ahead + (c + 1) * PER_CHUNK)
        return carry

    lax.fori_loop(0, n_chunk, step, 0)

    for c in (n_chunk - 2, n_chunk - 1):
        for cp in out_copies(c):
            cp.wait()

    @pl.when(me < last)
    def _():
        for j in range(per):
            rcopy(dh_ref.at[rows(j, C)], ds_ref.at[rows(me * per + j, C)], own_sem.at[j], recv_sem.at[me * per + j], last).wait_send()

    done = jnp.minimum(ahead + n_chunk * PER_CHUNK, n_unit)
    left = (n_unit - done + n_chunk - 1) // n_chunk

    def drain(c, carry):
        @pl.when(me > 0)
        def _():
            rcopy(ob.at[rows(c, C)], ds_ref.at[rows(c, C)], send_sem.at[c], recv_sem.at[c], prv).wait_send()
            rcopy(dx_ref.at[rows(c, C)], dx_ref.at[rows(c, C)], bsend.at[0, c], brecv.at[c], prv).wait_recv()
            spread(c, False)

        units(done + c * left, done + (c + 1) * left)
        return carry

    lax.fori_loop(0, n_chunk, drain, 0)
    for t in range(max(n_q - 2, 0), n_q):
        q_copy(t).wait()

    def settle(c, carry):
        spread(c, True)
        return carry

    lax.fori_loop(0, n_chunk, settle, 0)
    dx_ref[n_rows:, :] = jnp.zeros((WIN, dx_ref.shape[1]), BF)


def backward(S, C, tile, row0, tv, pre, dh, xs, w_in, w_in_t, w_out_t, nall, lse, tgt, emb, after):
    own, D = dh.shape
    n_rows = xs.shape[0]
    F = w_in.shape[1]
    n_chunk, per = n_rows // C, own // C
    n_q = pl.cdiv(emb.shape[0] - row0, tv)
    return pl.pallas_call(
        functools.partial(bwd_kernel, S, C, tile, row0, pre),
        out_shape=(jax.ShapeDtypeStruct((n_rows, D), BF), jax.ShapeDtypeStruct((n_rows, F), BF),
                   jax.ShapeDtypeStruct((n_rows, F), BF), jax.ShapeDtypeStruct((n_rows + WIN, D), BF),
                   jax.ShapeDtypeStruct((n_q * tv, D), F32)),
        in_specs=[VMEM] * 8 + [ANY] * 2,
        out_specs=(VMEM, ANY, ANY, VMEM, ANY),
        scratch_shapes=[
            pltpu.VMEM((n_rows, D), BF),
            pltpu.VMEM((2, C, F), BF),
            pltpu.VMEM((2, C, F), BF),
            pltpu.VMEM((2, tv, D), BF),
            pltpu.VMEM((2, tv, D), F32),
            pltpu.SemaphoreType.DMA((2,)),
            pltpu.SemaphoreType.DMA((2,)),
            pltpu.SemaphoreType.DMA((per,)),
            pltpu.SemaphoreType.DMA((n_chunk,)),
            pltpu.SemaphoreType.DMA((n_chunk,)),
            pltpu.SemaphoreType.DMA((2,)),
            pltpu.SemaphoreType.DMA((2,)),
            pltpu.SemaphoreType.DMA((3, n_chunk)),
            pltpu.SemaphoreType.DMA((n_chunk,)),
        ],
        compiler_params=pltpu.CompilerParams(collective_id=2, has_side_effects=True, vmem_limit_bytes=VMEM_MAX),
        cost_estimate=cost(n_rows * w_in.size, n_rows * F),
        name='bwd_pipe',
    )(dh, xs, w_in, w_in_t, w_out_t, nall, lse, tgt, emb, after)


def head_block(et, base, rows_j, lse_j, tgt_j):
    D = et.shape[1]
    k = 0.5 * D ** -0.5
    q = jnp.exp2(mm_t(et, rows_j) * (D ** -0.5 * math.log2(math.e)) - (lse_j - math.log2(k)))
    hit = lax.broadcasted_iota(jnp.int32, q.shape, 0) == tgt_j - base
    return mm(jnp.where(hit, q - k, q).astype(BF), rows_j)


def shard_kernel(off_ref, e_ref, nall_ref, lse_ref, tgt_ref, after_ref, o_ref):
    tv = e_ref.shape[0]
    nb, _, tb = lse_ref.shape
    base = (off_ref[0] + pl.program_id(0)) * tv
    o_ref[...] = head_block(e_ref[...], base, nall_ref[0:tb, :], lse_ref[0], tgt_ref[0])

    def body(j, carry):
        o_ref[...] += head_block(e_ref[...], base, nall_ref[rows(j, tb), :], lse_ref[j], tgt_ref[j])
        return carry

    lax.fori_loop(1, nb, body, 0)


def head_shard(tv, n_tile, off, emb, nall, lse, tgt, after):
    D = emb.shape[1]
    return pl.pallas_call(
        shard_kernel,
        out_shape=jax.ShapeDtypeStruct((n_tile * tv, D), F32),
        grid_spec=pltpu.PrefetchScalarGridSpec(
            num_scalar_prefetch=1, grid=(n_tile,),
            in_specs=[pl.BlockSpec((tv, D), lambda i, o: (o[0] + i, 0)), VMEM, VMEM, VMEM, ANY],
            out_specs=pl.BlockSpec((tv, D), lambda i, o: (i, 0))),
        compiler_params=pltpu.CompilerParams(vmem_limit_bytes=VMEM_MAX),
        cost_estimate=cost(n_tile * tv * nall.size, n_tile * tv * D),
        name='head_shard',
    )(off, emb, nall, lse, tgt, after)


def split3(v):
    hi = v.astype(BF)
    rest = v - hi.astype(F32)
    mid = rest.astype(BF)
    return [hi, mid, (rest - mid.astype(F32)).astype(BF)]


def place(t, parts):
    at, base = t, 0
    for first, n in parts:
        at = jnp.where(t >= base, first + t - base, at)
        base += n
    return at


def sweep_kernel(tv, parts, lim_ref, tokw_ref, dx_ref, labw_ref, dg_ref, *refs):
    a_refs, o_ref = refs[:len(parts)], refs[-1]
    t = pl.program_id(0)
    tile0 = place(t, parts) * SUB
    top = tokw_ref.shape[0] - 1

    def part(s, i):
        tile = jnp.minimum(tile0 + s, lim_ref.shape[1] - 1)
        wt = jnp.minimum(lim_ref[0, tile] + i * (WIN // STEP), top)
        wl = jnp.minimum(lim_ref[1, tile] + i * (WIN // STEP), top)
        ids = jnp.maximum(tokw_ref[pl.ds(wt, 1), :], labw_ref[pl.ds(wl, 1), :]) - (tile0 + s) * tv
        hit = lax.broadcasted_iota(jnp.int32, (tv, 4 * WIN), 0) == ids
        near = pl.ds(pl.multiple_of(wt * STEP, STEP), WIN)
        far = pl.ds(pl.multiple_of(wl * STEP, STEP), WIN)
        return mm(jnp.where(hit, 1.0, 0.0).astype(BF), jnp.concatenate([dx_ref[near, :]] + split3(dg_ref[far, :]), axis=0))

    base = 0
    for (first, n), a_ref in zip(parts, a_refs):
        @pl.when((t >= base) & (t < base + n))
        def _():
            for s in range(SUB):
                o_ref[s * tv:(s + 1) * tv, :] = a_ref[s * tv:(s + 1) * tv, :] + part(s, 0)

        base += n

    for s in range(SUB):
        def more(i, carry):
            o_ref[s * tv:(s + 1) * tv, :] += part(s, i)
            return carry

        lax.fori_loop(1, lim_ref[2, jnp.minimum(tile0 + s, lim_ref.shape[1] - 1)], more, 0)


def sweep(tv, parts, arrays, lim, tokw, dx, labw, dg, out_rows, full):
    D = dx.shape[1]
    size = SUB * tv
    keep = [] if full is None else [full]
    specs, base = [], 0
    for first, n in parts:
        specs.append(pl.BlockSpec((size, D), lambda t, base=base, n=n: (jnp.clip(t - base, 0, n - 1), 0)))
        base += n
    return pl.pallas_call(
        functools.partial(sweep_kernel, tv, parts),
        out_shape=jax.ShapeDtypeStruct((out_rows, D), F32),
        grid=(base,),
        in_specs=[SMEM] + [VMEM] * 4 + specs + [ANY] * len(keep),
        out_specs=pl.BlockSpec((size, D), lambda t: (place(t, parts), 0)),
        input_output_aliases={5 + len(parts): 0} if keep else {},
        compiler_params=pltpu.CompilerParams(vmem_limit_bytes=VMEM_MAX),
        cost_estimate=cost(base * size * D, base * size * D),
        name='sweep',
    )(lim, tokw, dx, labw, dg, *arrays, *keep)


def windows(sorted_ids, slots):
    pad = jnp.pad(sorted_ids, (0, WIN), constant_values=-1).reshape(-1, STEP)
    n = sorted_ids.size // STEP
    win = jnp.concatenate([pad[i:i + n] for i in range(WIN // STEP)], axis=1)
    none = jnp.full_like(win, -1)
    return jnp.pad(jnp.concatenate([win if s else none for s in slots], axis=1), ((0, 1), (0, 0)), constant_values=-1)


def limits(tok, lab, tv, n_tile):
    edge = jnp.arange(n_tile + 1, dtype=jnp.int32) * tv

    def span(ids):
        below = jnp.sum((ids[None, :] < edge[:, None]).astype(jnp.int32), axis=1)
        w = below[:-1] // STEP
        return w, (below[1:] - w * STEP + WIN - 1) // WIN

    wt, nt = span(tok)
    wl, nl = span(lab)
    return jnp.stack([wt, wl, jnp.maximum(nt, nl)])


TILE_V = 512
TOKENS = 1024
WIN = 64
STEP = 16
AHEAD = 4
PER_CHUNK = 1
SUB = 4
HALF_V = TILE_V // 2
PIECES = (4, 6, 3)
FWD_ROWS = 128
BWD_ROWS = 128


def solution(mesh):
    S = mesh.shape[AXIS]

    def per_device(token_ids, label_ids, label2_ids, embed_table, w_up, w_down, mtp_up, mtp_down):
        V, D = embed_table.shape
        N = token_ids.size
        R = N // S
        me = lax.axis_index(AXIS)
        w_in, w_out = w_up[0], w_down[0]

        tok, lab, lab2 = lax.sort((token_ids.reshape(N), label_ids.reshape(N), label2_ids.reshape(N)), num_keys=1)

        def own(v):
            return lax.dynamic_slice_in_dim(v, me * R, R)

        picked = embed_table[jnp.concatenate([own(tok), own(lab), own(lab2)])]
        x_own, e1, e2 = picked[:R], picked[R:2 * R], picked[2 * R:]
        xs, h_own, w_in_t, w_out_t = forward(S, FWD_ROWS, 1024, x_own, w_in, w_out)
        tg = jnp.concatenate([own(lab), own(lab2)]).reshape(2 * R, 1)
        nall, lall, st, lcol = lse_phase(S, 1024, 1024, h_own, e1, e2, mtp_up, mtp_down, embed_table)
        nall = nall.reshape(2 * N, D)
        lse = lall[:, 0, :].reshape(2 * N // TOKENS, 1, TOKENS)
        tgt = jnp.stack([lab.reshape(S, R), lab2.reshape(S, R)], axis=1).reshape(2 * N // TOKENS, 1, TOKENS)

        starts = [S * sum(PIECES[:i]) * HALF_V // TILE_V for i in range(len(PIECES) + 1)]

        def piece(i, after):
            tv = HALF_V if PIECES[i] % 2 else TILE_V
            n = PIECES[i] * HALF_V // tv
            off = (starts[i] * TILE_V // tv + me * n).reshape(1)
            return head_shard(tv, n, off, embed_table, nall, lse, tgt, after)

        def share(v):
            return lax.all_gather(v, AXIS, axis=0, tiled=True)

        mine = [piece(0, lcol)]
        gathered = [share(mine[0])]
        dh, dg = grad_phase(1024, 1024, st, e1, tg, lcol, mtp_up, mtp_down, embed_table, mine[0])
        for i in range(1, len(PIECES)):
            mine.append(piece(i, dg if i == 1 else mine[-1]))
            gathered.append(share(mine[-1]))
            if i == 1:
                dg_all = share(dg)

        dsv, dpre, hid, dx, q_part = backward(S, BWD_ROWS, 1024, starts[-1] * TILE_V, TILE_V, AHEAD, dh, xs, w_in, w_in_t, w_out_t, nall, lse, tgt, embed_table, mine[-1])
        g_up = lax.dot_general(xs, dpre, (((0,), (0,)), ((), ())), preferred_element_type=F32)
        g_down = lax.dot_general(hid, dsv, (((0,), (0,)), ((), ())), preferred_element_type=F32)
        loss = (0.5 * jnp.sum(lall[:, 1, 0]) / N).reshape(1)

        lab_sorted, lab_perm = lax.sort((lab, lax.iota(jnp.int32, N)), num_keys=1)
        dg_rows = dg_all[jnp.pad(lab_perm, (0, WIN))]
        n_tile = pl.cdiv(V, TILE_V)
        lim = limits(tok, lab_sorted, TILE_V, n_tile)
        tokw = windows(tok, (1, 0, 0, 0))
        labw = windows(lab_sorted, (0, 1, 1, 1))
        ends = starts[1:] + [pl.cdiv(n_tile, SUB) * SUB]
        span = [(a // SUB, (b - a) // SUB) for a, b in zip(starts, ends)]
        early = [0, 1, len(PIECES)]
        stock = gathered + [q_part]
        full = sweep(TILE_V, [span[i] for i in early], [stock[i] for i in early], lim, tokw, dx, labw, dg_rows, V, None)
        for i in range(2, len(PIECES)):
            full = sweep(TILE_V, [span[i]], [stock[i]], lim, tokw, dx, labw, dg_rows, V, full)
        return loss, g_up[None], g_down[None], full

    in_specs = (P('dp'),) * 3 + (P(), P('stage'), P('stage'), P(), P())
    out_specs = (P('dp'), P(('dp', 'stage')), P(('dp', 'stage')), P('dp'))
    return jax.shard_map(per_device, mesh=mesh, in_specs=in_specs, out_specs=out_specs, check_vma=False)
```
